32 devices in a mesh: gx: 2 (over core), gy: 4 (over y, x), ma: 4 (over z).
Axes of the slice: x: 2, y: 2, z: 4, core: 2. Of those that a mesh axis runs over, the one named last changes fastest.
Arguments:
- object_field: float32 [2, 256, 1024], P(None, 'gx', 'gy'), may hold values from -5 to 5
- probe_modes: float32 [8, 2, 256, 256], P('ma'), may hold values from -1.5 to 1.5
- measured: float32 [2, 4, 2, 256, 256], P('gx', 'gy'), may hold values from 0.1 to 4
- positions: int32 [2, 4, 2, 2], P('gx', 'gy'), may hold values from 0 to 255, as said below
- slot_counts: int32 [2, 4], P('gx', 'gy'), may hold values from 1 to 2, as said below
Outputs:
- updated_object: float32 [2, 256, 1024], P(None, 'gx', 'gy')
The draws below stay inside these ranges and needn't reach their ends.
Inputs may be any that keep to these rules, and one draw needn't show every extreme that they name: positions[a, b, s] holds a row 0 to 127 and a column 0 to 255 of tile (a, b); slots s >= slot_counts[a, b] are unused. `slot_counts`: some tile uses all 2 slots.
All inputs are finite; a program needn't handle non-finite values.
Results may differ from the reference program's by a relative error of at most 0.0023.
Values sent between devices are 32-bit elements; how exact they have to be, the bound alone decides.
No kernel may reach another device: no remote copies, remote signals or barrier semaphores. Data moves between devices by JAX's collectives and lax.ppermute only.
A program may use at most 64 MiB of HBM per device.

```python
import math
import jax
import jax.numpy as jnp
from jax import lax

PATCH = 256
MODES = 8
TX = 128
TY = 256
CAP = 2
OUTER = 2
ITERS = 1
GRID_X = 2
GRID_Y = 4
NX = 256
NY = 1024


def draw_positions(key, part):
    row_draw = jax.random.randint(jax.random.fold_in(key, 11), (GRID_X, GRID_Y, CAP, 1), 0, TX, dtype=jnp.int32)
    col_draw = jax.random.randint(jax.random.fold_in(key, 12), (GRID_X, GRID_Y, CAP, 1), 0, TY, dtype=jnp.int32)
    return jnp.concatenate([row_draw, col_draw], -1).astype(jnp.int32)


def draw_slot_counts(key, part):
    base_counts = jax.random.randint(jax.random.fold_in(key, 21), (GRID_X, GRID_Y), 1, CAP + 1, dtype=jnp.int32)
    chosen = jax.random.randint(jax.random.fold_in(key, 22), (), 0, GRID_X * GRID_Y, dtype=jnp.int32)
    tile_ids = jnp.arange(GRID_X * GRID_Y, dtype=jnp.int32).reshape(GRID_X, GRID_Y)
    return jnp.where(tile_ids == chosen, CAP, base_counts).astype(jnp.int32)


def level_of(key, shape, pieces, least, top_value):
    gain, own = 1.0, jax.random.fold_in(key, 6)
    for dim, blocks in pieces:
        heights = jnp.exp(jax.random.uniform(jax.random.fold_in(own, dim), (blocks,), jnp.float32, least / len(pieces), top_value / len(pieces)))
        gain = gain * jnp.repeat(heights, shape[dim] // blocks).reshape([-1 if axis == dim else 1 for axis in range(len(shape))])
    return gain


def noise(stream_key, extent, deviation, reach, pieces=(), kind=jnp.bfloat16):
    values = jax.random.normal(stream_key, extent, jnp.float32) * deviation
    if len(pieces) > 0:
        values = level_of(stream_key, extent, pieces, -0.22, 0.18) * values
    return jnp.clip(values, min=-reach, max=reach).astype(kind)


def setup_inputs(seed: int = 0) -> dict:
    streams_of = jax.random.split(jax.random.key(seed), 6)
    object_field = noise(streams_of[0], (2, NX, NY), 0.7, 5.0, ((1, 2), (2, 4)), jnp.float32)
    probe_modes = noise(streams_of[1], (MODES, 2, PATCH, PATCH), 0.25, 1.5, ((0, 4),), jnp.float32)
    measured = jnp.clip(jnp.exp(math.log(4.0) - 3.6888794 * jax.random.uniform(streams_of[2], (GRID_X, GRID_Y, CAP, PATCH, PATCH), jnp.float32) ** level_of(streams_of[2], (GRID_X, GRID_Y, CAP, PATCH, PATCH), ((0, 2), (1, 4)), -0.2, 0.2)), 0.1, 4.0)
    positions = draw_positions(jax.random.fold_in(streams_of[5], 71), 0)
    slot_counts = draw_slot_counts(jax.random.fold_in(streams_of[5], 71), 0)
    return {"object_field": object_field, "probe_modes": probe_modes, "measured": measured, "positions": positions, "slot_counts": slot_counts}


DAMPING = 1.0

def dft_tables(patch_width):
    ladder = jnp.arange(patch_width, dtype=jnp.int32)
    phases = ladder[:, None] * ladder[None, :] % patch_width
    angles = phases.astype(jnp.float32) * (2.0 * math.pi / patch_width)
    factor = 1.0 / math.sqrt(patch_width)
    real_part = jnp.cos(angles) * factor
    imag_part = -jnp.sin(angles) * factor
    table_one = jnp.concatenate([jnp.concatenate([real_part, -imag_part], 1), jnp.concatenate([imag_part, real_part], 1)], 0).astype(jnp.bfloat16)
    table_two = jnp.concatenate([jnp.concatenate([real_part, imag_part], 1), jnp.concatenate([-imag_part, real_part], 1)], 0).astype(jnp.bfloat16)
    return (table_one, table_two)

def forward_ref(wavefield, tables):
    patch_width = wavefield.shape[-1]
    first_table = tables[0].astype(jnp.float32).reshape(2, patch_width, 2, patch_width)
    second_table = tables[1].astype(jnp.float32).reshape(2, patch_width, 2 * patch_width)
    halfway = jnp.einsum('pqci,bcik->bpqk', first_table, wavefield.astype(jnp.float32)).astype(jnp.bfloat16)
    halfway = lax.optimization_barrier(halfway)
    return jnp.einsum('bcik,ckl->bil', halfway.astype(jnp.float32), second_table)

def adjoint_ref(weighted, tables):
    patch_width = weighted.shape[1]
    halfway = jnp.einsum('bik,kl->bil', weighted.astype(jnp.float32), tables[0].astype(jnp.float32)).astype(jnp.bfloat16)
    halfway = lax.optimization_barrier(halfway)
    second_table = tables[1].astype(jnp.float32).reshape(2, patch_width, 2, patch_width)
    return jnp.einsum('pqci,bicl->bpql', second_table, halfway.astype(jnp.float32).reshape(halfway.shape[0], patch_width, 2, patch_width))

def exit_waves(probe_modes, windows):
    probe_real = probe_modes[None, :, 0]
    probe_imag = probe_modes[None, :, 1]
    window_real = windows[:, None, 0]
    window_imag = windows[:, None, 1]
    real_part = probe_real * window_real - probe_imag * window_imag
    imag_part = probe_real * window_imag + probe_imag * window_real
    wavefield = jnp.stack([real_part, imag_part], 2).astype(jnp.bfloat16)
    wavefield = lax.optimization_barrier(wavefield)
    return wavefield.reshape(-1, 2, probe_modes.shape[-1], probe_modes.shape[-1])

def intensity_part(spectra, mode_count):
    patch_width = spectra.shape[1]
    grouped = spectra.reshape(-1, mode_count, patch_width, 2 * patch_width)
    squared = grouped * grouped
    return lax.optimization_barrier(jnp.sum(squared[..., :patch_width] + squared[..., patch_width:], axis=1))

def change_part(spectra, moved_spectra, mode_count):
    patch_width = spectra.shape[1]
    grouped = spectra.reshape(-1, mode_count, patch_width, 2 * patch_width)
    shifted = moved_spectra.reshape(-1, mode_count, patch_width, 2 * patch_width)
    product = grouped * shifted
    return 2.0 * lax.optimization_barrier(jnp.sum(product[..., :patch_width] + product[..., patch_width:], axis=1))

def mode_images(weights, spectra, probe_modes, tables):
    mode_count = probe_modes.shape[0]
    patch_width = probe_modes.shape[-1]
    doubled = jnp.concatenate([weights, weights], -1)
    grouped = spectra.reshape(-1, mode_count, patch_width, 2 * patch_width)
    weighted = (2.0 * grouped * doubled[:, None]).astype(jnp.bfloat16)
    weighted = lax.optimization_barrier(weighted)
    returned = adjoint_ref(weighted.reshape(-1, patch_width, 2 * patch_width), tables)
    returned = returned.reshape(-1, mode_count, 2, patch_width, patch_width)
    probe_real = probe_modes[None, :, 0]
    probe_imag = probe_modes[None, :, 1]
    real_part = lax.optimization_barrier(jnp.sum(probe_real * returned[:, :, 0] + probe_imag * returned[:, :, 1], axis=1))
    imag_part = lax.optimization_barrier(jnp.sum(probe_real * returned[:, :, 1] - probe_imag * returned[:, :, 0], axis=1))
    return jnp.stack([real_part, imag_part], 1)

def reference(object_field, probe_modes, measured, positions, slot_counts):
    half_width = PATCH // 2
    tables = dft_tables(PATCH)
    first_rows = (jnp.arange(GRID_X, dtype=jnp.int32) * TX)[:, None, None]
    first_cols = (jnp.arange(GRID_Y, dtype=jnp.int32) * TY)[None, :, None]
    corner_rows = (positions[..., 0] + first_rows).reshape(-1).astype(jnp.int32)
    corner_cols = (positions[..., 1] + first_cols).reshape(-1).astype(jnp.int32)
    corners = jnp.stack([corner_rows, corner_cols], 1)
    live_mask = (jnp.arange(CAP, dtype=jnp.int32)[None, None, :] < slot_counts[:, :, None]).astype(jnp.float32).reshape(-1)[:, None, None]
    targets = measured.reshape(-1, PATCH, PATCH)
    anchor = jnp.zeros((), jnp.int32)

    def padded_of(current):
        return jnp.pad(current, ((0, 0), (half_width, half_width), (half_width, half_width)))

    def spectra_of(current):
        padded = padded_of(current)

        def one_pattern(corner):
            window = lax.dynamic_slice(padded, (anchor, corner[0], corner[1]), (2, PATCH, PATCH))
            return forward_ref(exit_waves(probe_modes, window[None]), tables)
        return lax.map(one_pattern, corners)

    def project(weights, spectra):
        canvas = jnp.zeros((2, NX + PATCH, NY + PATCH), jnp.float32)

        def place(canvas, inputs):
            corner, weight, spectrum = inputs
            piece = mode_images(weight[None], spectrum, probe_modes, tables)[0]
            where = (anchor, corner[0], corner[1])
            canvas = lax.dynamic_update_slice(canvas, lax.dynamic_slice(canvas, where, (2, PATCH, PATCH)) + piece, where)
            return (canvas, None)
        canvas = lax.scan(place, canvas, (corners, weights, spectra))[0]
        return canvas[:, half_width:half_width + NX, half_width:half_width + NY]
    current = object_field
    for outer_step in range(OUTER):
        spectra = spectra_of(current)

        def one_intensity(spectrum):
            return intensity_part(spectrum, MODES)[0]
        intensity = lax.map(one_intensity, spectra)
        misfit = live_mask * (intensity - targets)
        gradient = project(misfit, spectra)

        def operator(vector):
            padded = padded_of(vector)

            def one_change(inputs):
                corner, spectrum = inputs
                window = lax.dynamic_slice(padded, (anchor, corner[0], corner[1]), (2, PATCH, PATCH))
                moved_spectra = forward_ref(exit_waves(probe_modes, window[None]), tables)
                return change_part(spectrum, moved_spectra, MODES)[0]
            change = live_mask * lax.map(one_change, (corners, spectra))
            return project(change, spectra) + DAMPING * vector
        update = jnp.zeros_like(current)
        residual = -gradient
        direction = residual
        norm_now = jnp.sum(residual * residual)
        for inner_step in range(ITERS):
            applied = operator(direction)
            step_size = norm_now / jnp.sum(direction * applied)
            update = update + step_size * direction
            residual = residual - step_size * applied
            if inner_step + 1 < ITERS:
                norm_next = jnp.sum(residual * residual)
                direction = residual + norm_next / norm_now * direction
                norm_now = norm_next
        current = current + update
    return current
```

```python
import math

import jax
import jax.numpy as jnp
from jax import lax
from jax.sharding import PartitionSpec as P

OUTER = 2


DAMPING = 1.0


def dft_tables(patch_width):
    ladder = jnp.arange(patch_width, dtype=jnp.int32)
    phases = ladder[:, None] * ladder[None, :] % patch_width
    angles = phases.astype(jnp.float32) * (2.0 * math.pi / patch_width)
    factor = 1.0 / math.sqrt(patch_width)
    real_part = jnp.cos(angles) * factor
    imag_part = -jnp.sin(angles) * factor
    table_one = jnp.concatenate(
        [jnp.concatenate([real_part, -imag_part], 1), jnp.concatenate([imag_part, real_part], 1)], 0
    ).astype(jnp.bfloat16)
    table_two = jnp.concatenate(
        [jnp.concatenate([real_part, imag_part], 1), jnp.concatenate([-imag_part, real_part], 1)], 0
    ).astype(jnp.bfloat16)
    return (table_one, table_two)


def forward_transform(wavefield, tables):
    patch_width = wavefield.shape[-1]
    halfway = jnp.einsum(
        "pqci,bcik->bpqk",
        tables[0].reshape(2, patch_width, 2, patch_width),
        wavefield,
        preferred_element_type=jnp.float32,
    ).astype(jnp.bfloat16)
    return jnp.einsum(
        "bcik,ckl->bil",
        halfway,
        tables[1].reshape(2, patch_width, 2 * patch_width),
        preferred_element_type=jnp.float32,
    )


def adjoint_transform(weighted, tables):
    patch_width = weighted.shape[1]
    halfway = jnp.einsum(
        "bik,kl->bil", weighted, tables[0], preferred_element_type=jnp.float32
    ).astype(jnp.bfloat16)
    return jnp.einsum(
        "pqci,bicl->bpql",
        tables[1].reshape(2, patch_width, 2, patch_width),
        halfway.reshape(halfway.shape[0], patch_width, 2, patch_width),
        preferred_element_type=jnp.float32,
    )


def exit_waves(probe_modes, windows):
    probe_real = probe_modes[None, :, 0]
    probe_imag = probe_modes[None, :, 1]
    window_real = windows[:, None, 0]
    window_imag = windows[:, None, 1]
    real_part = probe_real * window_real - probe_imag * window_imag
    imag_part = probe_real * window_imag + probe_imag * window_real
    wavefield = jnp.stack([real_part, imag_part], 2).astype(jnp.bfloat16)
    return wavefield.reshape(-1, 2, probe_modes.shape[-1], probe_modes.shape[-1])


def paired_sum(first, second, mode_count):
    patch_width = first.shape[1]
    product = (first * second).reshape(-1, mode_count, patch_width, 2 * patch_width)
    return jnp.sum(product[..., :patch_width] + product[..., patch_width:], axis=1)


def mode_images(weights, spectra, probe_modes, tables):
    mode_count = probe_modes.shape[0]
    patch_width = probe_modes.shape[-1]
    doubled = jnp.concatenate([weights, weights], -1)
    grouped = spectra.reshape(-1, mode_count, patch_width, 2 * patch_width)
    weighted = (2.0 * grouped * doubled[:, None]).astype(jnp.bfloat16)
    returned = adjoint_transform(weighted.reshape(-1, patch_width, 2 * patch_width), tables)
    returned = returned.reshape(-1, mode_count, 2, patch_width, patch_width)
    probe_real = probe_modes[None, :, 0]
    probe_imag = probe_modes[None, :, 1]
    real_part = jnp.sum(probe_real * returned[:, :, 0] + probe_imag * returned[:, :, 1], axis=1)
    imag_part = jnp.sum(probe_real * returned[:, :, 1] - probe_imag * returned[:, :, 0], axis=1)
    return jnp.stack([real_part, imag_part], 1)


def pair_swaps(count):
    even = [(i, i ^ 1) for i in range(count) if (i ^ 1) < count]
    if count < 3:
        return even, None
    odd = [(i, i + 1) for i in range(1, count - 1, 2)]
    if count % 2 == 0:
        odd = odd + [(count - 1, 0)]
    return even, odd + [(target, source) for source, target in odd]


def neighbours(axis, block, dim, low_start, high_start, width):
    count = lax.axis_size(axis)
    place = lax.axis_index(axis)
    is_even = place % 2 == 0
    even, odd = pair_swaps(count)

    def piece(start):
        return lax.dynamic_slice_in_dim(block, start, width, dim)

    first = lax.ppermute(piece(jnp.where(is_even, high_start, low_start)), axis, even)
    if odd is None:
        second = jnp.zeros_like(first)
    else:
        second = lax.ppermute(piece(jnp.where(is_even, low_start, high_start)), axis, odd)
    from_high = jnp.where(place + 1 < count, jnp.where(is_even, first, second), 0.0)
    from_low = jnp.where(place > 0, jnp.where(is_even, second, first), 0.0)
    return from_low, from_high


def gather_modes(probe_modes, axis):
    count = lax.axis_size(axis)
    place = lax.axis_index(axis)
    half = lax.axis_index("gx") % 2
    even, _ = pair_swaps(lax.axis_size("gx"))
    lead = probe_modes.shape[0]
    rows = probe_modes.reshape(lead * 2, *probe_modes.shape[2:])
    width = rows.shape[1] // 2
    mine = lax.dynamic_slice_in_dim(rows, half * width, width, 1)
    parts = [mine]
    for step in range(1, count):
        parts.append(
            lax.ppermute(mine, axis, [(i, (i + step) % count) for i in range(count)])
        )
    held = jnp.stack(parts, 0)
    others = lax.ppermute(held, "gx", even)
    low = jnp.where(half == 0, held, others)
    high = jnp.where(half == 0, others, held)
    whole = jnp.concatenate([low, high], 2)
    order = (place - jnp.arange(count)) % count
    whole = jnp.take(whole, order, axis=0)
    return whole.reshape(count * lead, *probe_modes.shape[1:])


def total(values):
    values = values + lax.ppermute(values, "gx", pair_swaps(lax.axis_size("gx"))[0]) if lax.axis_size(
        "gx"
    ) == 2 else lax.psum(values, "gx")
    count = lax.axis_size("gy")
    everyone = [values]
    for step in range(1, count):
        everyone.append(lax.ppermute(values, "gy", [(i, i ^ step) for i in range(count)]))
    place = lax.axis_index("gy")
    stacked = jnp.stack(everyone, 0)
    return jnp.sum(jnp.take(stacked, jnp.arange(count) ^ place, axis=0), axis=0)


def shards(object_field, probe_shard, measured, positions, slot_counts):
    patch_width = probe_shard.shape[-1]
    rim = patch_width // 2
    tile_rows = object_field.shape[1]
    tile_cols = object_field.shape[2]
    slot_count = measured.shape[2]
    tables = dft_tables(patch_width)
    targets = measured[0, 0]
    centres = positions[0, 0]
    live_mask = (jnp.arange(slot_count, dtype=jnp.int32) < slot_counts[0, 0]).astype(jnp.float32)[
        :, None, None
    ]
    probe_modes = gather_modes(probe_shard, "ma")
    mode_count = probe_modes.shape[0]

    def rows_around(block):
        low, high = neighbours("gx", block, 1, 0, tile_rows - rim, rim)
        return jnp.concatenate([low, block, high], 1)

    def windows_of(region):
        return jnp.stack(
            [
                lax.dynamic_slice(
                    region, (0, centres[s, 0], centres[s, 1]), (2, patch_width, patch_width)
                )
                for s in range(slot_count)
            ],
            0,
        )

    def spectra_of(region):
        return forward_transform(exit_waves(probe_modes, windows_of(region)), tables)

    def gather_image(pieces):
        canvas = 0.0
        for s in range(slot_count):
            spread = jnp.pad(pieces[s], ((0, 0), (tile_rows, tile_rows), (tile_cols, tile_cols)))
            canvas = canvas + lax.dynamic_slice(
                spread,
                (0, tile_rows - centres[s, 0], tile_cols - centres[s, 1]),
                (2, tile_rows + patch_width, tile_cols + patch_width),
            )
        low, high = neighbours("gx", canvas, 1, 0, tile_rows + rim, rim)
        middle = canvas[:, rim : rim + tile_rows]
        edge = ((0, 0), (0, tile_rows - rim), (0, 0))
        other = ((0, 0), (tile_rows - rim, 0), (0, 0))
        middle = middle + jnp.pad(low, edge) + jnp.pad(high, other)
        low, high = neighbours("gy", middle, 2, 0, tile_cols, patch_width)
        gap = tile_cols - patch_width
        place = lax.axis_index("gy")
        column = jnp.arange(tile_cols + patch_width)
        inside = (column >= jnp.where(place == 0, rim, 0)) & (
            column
            < jnp.where(place == lax.axis_size("gy") - 1, rim + tile_cols, tile_cols + patch_width)
        )
        widened = (
            middle
            + jnp.pad(low, ((0, 0), (0, 0), (0, gap + patch_width)))
            + jnp.pad(high, ((0, 0), (0, 0), (gap + patch_width, 0)))
        )
        return jnp.where(inside, widened, 0.0)

    low, high = neighbours("gy", object_field, 2, 0, tile_cols - rim, rim)
    start_region = rows_around(jnp.concatenate([low, object_field, high], 2))
    current = object_field
    spectra = spectra_of(start_region)
    intensity = paired_sum(spectra, spectra, mode_count)
    for outer_step in range(OUTER):
        misfit = live_mask * (intensity - targets)
        descent = -gather_image(mode_images(misfit, spectra, probe_modes, tables))
        direction = descent[:, :, rim : rim + tile_cols]
        moved = spectra_of(rows_around(descent))
        change = 2.0 * paired_sum(spectra, moved, mode_count)
        partial = jnp.stack([jnp.sum(direction * direction), jnp.sum(live_mask * change * change)])
        sums = total(partial)
        step_size = sums[0] / (sums[1] + DAMPING * sums[0])
        current = current + step_size * direction
        if outer_step + 1 < OUTER:
            power = paired_sum(moved, moved, mode_count)
            spectra = spectra + step_size * moved
            intensity = intensity + step_size * (change + step_size * power)
    return current


def solution(mesh):
    return jax.shard_map(
        shards,
        mesh=mesh,
        in_specs=(
            P(None, "gx", "gy"),
            P("ma", None, None, None),
            P("gx", "gy", None, None, None),
            P("gx", "gy", None, None),
            P("gx", "gy"),
        ),
        out_specs=P(None, "gx", "gy"),
        check_vma=False,
    )
```

```python
import functools
import math

import jax
import jax.numpy as jnp
import ml_dtypes
import numpy as np
from jax import lax
from jax.experimental import pallas as pl
from jax.experimental.pallas import tpu as pltpu
from jax.sharding import PartitionSpec as P

DAMPING = 1.0
UNROLL = 2


def dft_tables(width):
    ladder = np.arange(width, dtype=np.int64)
    angles = (ladder[:, None] * ladder[None, :] % width) * (2.0 * math.pi / width)
    real_part = np.cos(angles) / math.sqrt(width)
    imag_part = -np.sin(angles) / math.sqrt(width)
    table_one = np.block([[real_part, -imag_part], [imag_part, real_part]])
    table_two = np.block([[real_part, imag_part], [-imag_part, real_part]])
    return table_one.astype(ml_dtypes.bfloat16), table_two.astype(ml_dtypes.bfloat16)


def pair_swaps(count):
    even = [(i, i ^ 1) for i in range(count) if (i ^ 1) < count]
    if count < 3:
        return [even]
    odd = [(i, i + 1) for i in range(1, count - 1, 2)]
    if count % 2 == 0:
        odd = odd + [(count - 1, 0)]
    return [even, odd + [(target, source) for source, target in odd]]


def side_weights(axis):
    count = lax.axis_size(axis)
    place = lax.axis_index(axis)
    even = place % 2 == 0
    has_low = place > 0
    has_high = place + 1 < count
    flags = [even & has_high, ~even & has_low]
    if count > 2:
        flags = [~even & has_low, even & has_low, even & has_high, ~even & has_high]
    else:
        flags = [~even & has_low, even & has_high]
    return jnp.stack(flags).astype(jnp.float32)


def swap(axis, blocks):
    return [
        lax.ppermute(block, axis, pairs)
        for block, pairs in zip(blocks, pair_swaps(lax.axis_size(axis)))
    ]


def dot(left, right):
    return jnp.dot(left, right, preferred_element_type=jnp.float32)


def call(body, name, out_shapes, in_spaces, operands, out_spaces=None, scratch=()):
    specs = [pl.BlockSpec(memory_space=space) for space in in_spaces]
    out_spaces = out_spaces or [pltpu.VMEM] * len(out_shapes)
    return pl.pallas_call(
        body,
        name=name,
        out_shape=[jax.ShapeDtypeStruct(shape, jnp.float32) for shape in out_shapes],
        in_specs=specs,
        out_specs=[pl.BlockSpec(memory_space=space) for space in out_spaces],
        scratch_shapes=list(scratch),
        compiler_params=pltpu.CompilerParams(vmem_limit_bytes=60 * 2**20),
    )(*operands)


class Plan:
    def __init__(self, tile_rows, tile_cols, patch, modes, slots):
        self.tile_rows, self.tile_cols = tile_rows, tile_cols
        self.patch, self.modes, self.slots = patch, modes, slots
        self.rim = patch // 2
        self.rows = tile_rows + patch
        self.cols = tile_cols + patch

    def scratch(self):
        wide = self.patch
        return [
            pltpu.VMEM((2, self.rows, self.cols), jnp.float32),
            pltpu.VMEM((self.slots, 2, wide, wide), jnp.float32),
            pltpu.VMEM((UNROLL, 2 * wide, wide), jnp.bfloat16),
            pltpu.VMEM((UNROLL, 2 * wide, wide), jnp.bfloat16),
        ]

    def fill_region(self, region, middle, received, weights):
        rim, rows = self.rim, self.tile_rows
        count = len(received)
        low = sum(received[k][...] * weights[k] for k in range(count))
        high = sum(received[k][...] * weights[count + k] for k in range(count))
        region[:, :rim] = low
        region[:, rim : rim + rows] = middle[...]
        region[:, rim + rows :] = high

    def row_split(self, row):
        shift = lax.rem(row, 8)
        return pl.multiple_of(row - shift, 8), shift

    def take_windows(self, windows, region, centres):
        wide = self.patch
        for slot in range(self.slots):
            for part in range(2):
                base, shift = self.row_split(centres[slot, 0])
                strip = region[part, pl.ds(base, wide + 8), :]
                strip = pltpu.roll(strip, wide + 8 - shift, 0)[:wide]
                turned = pltpu.roll(strip, self.cols - centres[slot, 1], 1)
                windows[slot, part] = turned[:, :wide]

    def place(self, canvas, slot, part, piece, centres):
        strip = jnp.concatenate([piece, jnp.zeros((self.patch, self.cols - self.patch), jnp.float32)], 1)
        strip = jnp.concatenate([strip, jnp.zeros((8, self.cols), jnp.float32)], 0)
        base, shift = self.row_split(centres[slot, 0])
        turned = pltpu.roll(pltpu.roll(strip, centres[slot, 1], 1), shift, 0)
        canvas[part, pl.ds(base, self.patch + 8), :] += turned

    def each_modes(self, slot, body):
        def step(index, carry):
            body([index * UNROLL + j for j in range(UNROLL)])
            return carry

        lax.fori_loop(0, self.modes // UNROLL, step, 0)

    def spectra(self, slot, modes, probes, windows, wave, half, tables):
        wide = self.patch
        x_real, x_imag = windows[slot, 0], windows[slot, 1]
        for j, mode in enumerate(modes):
            p_real, p_imag = probes[mode, 0], probes[mode, 1]
            wave[j, :wide] = (p_real * x_real - p_imag * x_imag).astype(jnp.bfloat16)
            wave[j, wide:] = (p_real * x_imag + p_imag * x_real).astype(jnp.bfloat16)
        for j in range(len(modes)):
            half[j] = dot(tables[0][...], wave[j]).astype(jnp.bfloat16)
        return [
            dot(half[j, :wide], tables[1][:wide]) + dot(half[j, wide:], tables[1][wide:])
            for j in range(len(modes))
        ]

    def images(self, fields, weight, modes, probes, wave, half, tables):
        wide = self.patch
        for j, field in enumerate(fields):
            half[j, :wide] = (2.0 * field[:, :wide] * weight).astype(jnp.bfloat16)
            half[j, wide:] = (2.0 * field[:, wide:] * weight).astype(jnp.bfloat16)
        for j in range(len(modes)):
            turned = dot(half[j, :wide], tables[0][:wide]) + dot(half[j, wide:], tables[0][wide:])
            turned = turned.astype(jnp.bfloat16)
            wave[j, :wide] = turned[:, :wide]
            wave[j, wide:] = turned[:, wide:]
        real_sum = imag_sum = 0.0
        for j, mode in enumerate(modes):
            back = dot(tables[1][...], wave[j])
            p_real, p_imag = probes[mode, 0], probes[mode, 1]
            real_sum = real_sum + (p_real * back[:wide] + p_imag * back[wide:])
            imag_sum = imag_sum + (p_real * back[wide:] - p_imag * back[:wide])
        return real_sum, imag_sum

    def send(self, canvas, parity, middle_out, sends):
        rim, rows = self.rim, self.tile_rows
        middle_out[...] = canvas[:, rim : rim + rows]
        for k, out in enumerate(sends):
            upper = parity[0] if k == 0 else 1 - parity[0]
            start = pl.multiple_of((1 - upper) * (rim + rows), 8)
            out[...] = canvas[:, pl.ds(start, rim), :]


def start_body(plan, swaps, shards, *refs):
    refs = list(refs)
    info, centres, weights, middle = refs[:4]
    received = refs[4 : 4 + swaps]
    shard, *rest = refs[4 + swaps : 4 + swaps + 2 * shards - 1]
    direct, crossed = rest[: shards - 1], rest[shards - 1 :]
    targets, one, two = refs[3 + swaps + 2 * shards : 6 + swaps + 2 * shards]
    spectra, intensity, probes, middle_out, *tail = refs[6 + swaps + 2 * shards :]
    sends = tail[:swaps]
    region, windows, wave, half, image = tail[swaps:]
    wide, lead = plan.patch, plan.modes // shards
    tables = (one, two)
    place, side = info[2], info[3]
    span = wide // 2

    probes[pl.ds(place * lead, lead)] = shard[...]
    for k in range(1, shards):
        home = lax.rem(place - k + shards, shards) * lead
        near = pl.multiple_of(side * span, 8)
        far = pl.multiple_of((1 - side) * span, 8)
        probes[pl.ds(home, lead), :, pl.ds(near, span), :] = direct[k - 1][...]
        probes[pl.ds(home, lead), :, pl.ds(far, span), :] = crossed[k - 1][...]

    plan.fill_region(region, middle, received, weights)
    plan.take_windows(windows, region, centres)
    region[...] = jnp.zeros_like(region)
    for slot in range(plan.slots):
        intensity[slot] = jnp.zeros((wide, wide), jnp.float32)

        def forward(modes):
            fields = plan.spectra(slot, modes, probes, windows, wave, half, tables)
            power = 0.0
            for mode, field in zip(modes, fields):
                spectra[slot * plan.modes + mode] = field
                power = power + (field[:, :wide] * field[:, :wide] + field[:, wide:] * field[:, wide:])
            intensity[slot] += power

        plan.each_modes(slot, forward)
        live = jnp.where(slot < info[0], 1.0, 0.0)
        windows[slot, 0] = live * (intensity[slot] - targets[slot])
        image[...] = jnp.zeros_like(image)

        def backward(modes):
            fields = [spectra[slot * plan.modes + mode] for mode in modes]
            real_sum, imag_sum = plan.images(fields, windows[slot, 0], modes, probes, wave, half, tables)
            image[0] += real_sum
            image[1] += imag_sum

        plan.each_modes(slot, backward)
        for part in range(2):
            plan.place(region, slot, part, image[part], centres)
    plan.send(region, [info[1]], middle_out, sends)


def change_body(plan, swaps, last, *refs):
    refs = list(refs)
    info, centres, weights, middle = refs[:4]
    received = refs[4 : 4 + swaps]
    spectra, probes, one, two = refs[4 + swaps : 8 + swaps]
    outs = refs[8 + swaps :]
    if last:
        sums, region, windows, wave, half, change, power = outs
    else:
        sums, moved, change, power, region, windows, wave, half = outs
    wide, rim = plan.patch, plan.rim
    tables = (one, two)
    plan.fill_region(region, middle, received, weights)
    plan.take_windows(windows, region, centres)
    own = middle[:, :, rim : rim + plan.tile_cols]
    sums[0] = jnp.sum(own * own)
    bend = 0.0
    for slot in range(plan.slots):
        change[slot] = jnp.zeros((wide, wide), jnp.float32)
        if not last:
            power[slot] = jnp.zeros((wide, wide), jnp.float32)

        def forward(modes):
            fields = plan.spectra(slot, modes, probes, windows, wave, half, tables)
            cross = square = 0.0
            for mode, field in zip(modes, fields):
                base = spectra[slot * plan.modes + mode]
                cross = cross + (base[:, :wide] * field[:, :wide] + base[:, wide:] * field[:, wide:])
                if not last:
                    moved[slot * plan.modes + mode] = field
                    square = square + (
                        field[:, :wide] * field[:, :wide] + field[:, wide:] * field[:, wide:]
                    )
            change[slot] += 2.0 * cross
            if not last:
                power[slot] += square

        plan.each_modes(slot, forward)
        live = jnp.where(slot < info[0], 1.0, 0.0)
        bend = bend + live * jnp.sum(change[slot] * change[slot])
    sums[1] = bend


def image_body(plan, swaps, parts, *refs):
    refs = list(refs)
    info, centres = refs[:2]
    totals = refs[2 : 2 + parts]
    spectra, moved, intensity, change, power, probes, targets, one, two = refs[2 + parts : 11 + parts]
    fresh, step_out, middle_out, *tail = refs[11 + parts :]
    sends = tail[:swaps]
    region, windows, wave, half, image = tail[swaps:]
    tables = (one, two)
    step = step_of(totals)
    step_out[0] = step
    region[...] = jnp.zeros_like(region)
    for slot in range(plan.slots):
        live = jnp.where(slot < info[0], 1.0, 0.0)
        bright = intensity[slot] + step * (change[slot] + step * power[slot])
        windows[slot, 0] = live * (bright - targets[slot])
        image[...] = jnp.zeros_like(image)

        def backward(modes):
            fields = []
            for mode in modes:
                field = spectra[slot * plan.modes + mode] + step * moved[slot * plan.modes + mode]
                fresh[slot * plan.modes + mode] = field
                fields.append(field)
            real_sum, imag_sum = plan.images(fields, windows[slot, 0], modes, probes, wave, half, tables)
            image[0] += real_sum
            image[1] += imag_sum

        plan.each_modes(slot, backward)
        for part in range(2):
            plan.place(region, slot, part, image[part], centres)
    plan.send(region, [info[1]], middle_out, sends)


def step_of(totals):
    values = [[part[k] for part in totals] for k in range(2)]
    while len(values[0]) > 1:
        values = [[v[i] + v[i + 1] for i in range(0, len(v), 2)] for v in values]
    norm, bend = values[0][0], values[1][0]
    top = jnp.full((8, 128), norm, jnp.float32)
    return jnp.max(top / (bend + DAMPING * norm))


def totals_of(sums):
    if lax.axis_size("gx") == 2:
        sums = sums + swap("gx", [sums])[0]
    else:
        sums = lax.psum(sums, "gx")
    count = lax.axis_size("gy")
    if count & (count - 1):
        return [lax.psum(sums, "gy")]
    return [sums] + [
        lax.ppermute(sums, "gy", [(i, i ^ step) for i in range(count)]) for step in range(1, count)
    ]


def shards(object_field, probe_shard, measured, positions, slot_counts):
    patch = probe_shard.shape[-1]
    tile_rows, tile_cols = object_field.shape[1:]
    groups = lax.axis_size("ma")
    modes = probe_shard.shape[0] * groups
    slots = measured.shape[2]
    plan = Plan(tile_rows, tile_cols, patch, modes, slots)
    rim, units = plan.rim, slots * modes
    one, two = (jnp.asarray(table) for table in dft_tables(patch))
    targets = measured[0, 0]
    centres = positions[0, 0]
    gx, gy, ma = (lax.axis_index(axis) for axis in ("gx", "gy", "ma"))
    even_x, even_y = gx % 2 == 0, gy % 2 == 0
    info = jnp.stack([slot_counts[0, 0], even_x.astype(jnp.int32) * 0 + gx % 2, ma, gx % 2])
    swaps_x, swaps_y = (len(pair_swaps(lax.axis_size(axis))) for axis in ("gx", "gy"))
    weights_x = side_weights("gx")
    smem, vmem = pltpu.SMEM, pltpu.VMEM
    tall = (2, tile_rows, plan.cols)
    fold = (2, rim, plan.cols)
    image_scratch = pltpu.VMEM((2, patch, patch), jnp.float32)

    def halves(block, dim, low_start, high_start, width, is_even, swaps):
        def piece(start):
            return lax.dynamic_slice_in_dim(block, start, width, dim)

        first = piece(jnp.where(is_even, high_start, low_start))
        return [first] + [piece(jnp.where(is_even, low_start, high_start))] * (swaps - 1)

    def rows_around(middle):
        if rim == tile_rows:
            return swap("gx", [middle] * swaps_x)
        return swap("gx", halves(middle, 1, 0, tile_rows - rim, rim, even_x, swaps_x))

    def sides(axis, received):
        weights = side_weights(axis)
        count = len(received)
        low = sum(received[k] * weights[k] for k in range(count))
        high = sum(received[k] * weights[count + k] for k in range(count))
        return low, high

    def descent(middle, sends):
        low, high = sides("gx", swap("gx", sends))
        gap = tile_rows - rim
        middle = middle + jnp.pad(low, ((0, 0), (0, gap), (0, 0)))
        middle = middle + jnp.pad(high, ((0, 0), (gap, 0), (0, 0)))
        blocks = halves(middle, 2, 0, tile_cols, patch, even_y, swaps_y)
        low, high = sides("gy", swap("gy", blocks))
        column = jnp.arange(plan.cols)
        first = jnp.where(gy == 0, rim, 0)
        final = jnp.where(gy == lax.axis_size("gy") - 1, rim + tile_cols, plan.cols)
        middle = middle + jnp.pad(low, ((0, 0), (0, 0), (0, tile_cols)))
        middle = middle + jnp.pad(high, ((0, 0), (0, 0), (tile_cols, 0)))
        return jnp.where((column >= first) & (column < final), -middle, 0.0)

    def own(middle):
        return middle[:, :, rim : rim + tile_cols]

    span = patch // 2
    mine = lax.dynamic_slice_in_dim(probe_shard, (gx % 2) * span, span, 2)
    direct = [
        lax.ppermute(mine, "ma", [(i, (i + k) % groups) for i in range(groups)])
        for k in range(1, groups)
    ]
    crossed = [swap("gx", [block])[0] for block in direct]

    blocks = halves(object_field, 2, 0, tile_cols - rim, rim, even_y, swaps_y)
    low, high = sides("gy", swap("gy", blocks))
    middle = jnp.concatenate([low, object_field, high], 2)

    spectra, intensity, probes, middle, *sends = call(
        functools.partial(start_body, plan, swaps_x, groups),
        "start",
        [(units, patch, 2 * patch), (slots, patch, patch), (modes, 2, patch, patch), tall]
        + [fold] * swaps_x,
        [smem] * 3 + [vmem] * (1 + swaps_x + 2 * groups - 1 + 3),
        [info, centres, weights_x, middle, *rows_around(middle), probe_shard]
        + direct
        + crossed
        + [targets, one, two],
        scratch=plan.scratch() + [image_scratch],
    )
    middle = descent(middle, sends)
    sums, moved, change, power = call(
        functools.partial(change_body, plan, swaps_x, False),
        "change",
        [(2,), (units, patch, 2 * patch), (slots, patch, patch), (slots, patch, patch)],
        [smem] * 3 + [vmem] * (5 + swaps_x),
        [info, centres, weights_x, middle, *rows_around(middle), spectra, probes, one, two],
        [smem] + [vmem] * 3,
        scratch=plan.scratch(),
    )
    first_way = own(middle)
    totals = totals_of(sums)
    spectra, first_step, middle, *sends = call(
        functools.partial(image_body, plan, swaps_x, len(totals)),
        "image",
        [(units, patch, 2 * patch), (1,), tall] + [fold] * swaps_x,
        [smem] * (2 + len(totals)) + [vmem] * 9,
        [info, centres, *totals, spectra, moved, intensity, change, power, probes, targets, one, two],
        [vmem, smem] + [vmem] * (1 + swaps_x),
        scratch=plan.scratch() + [image_scratch],
    )
    middle = descent(middle, sends)
    (sums,) = call(
        functools.partial(change_body, plan, swaps_x, True),
        "last_change",
        [(2,)],
        [smem] * 3 + [vmem] * (5 + swaps_x),
        [info, centres, weights_x, middle, *rows_around(middle), spectra, probes, one, two],
        [smem],
        scratch=plan.scratch()
        + [pltpu.VMEM((slots, patch, patch), jnp.float32), pltpu.VMEM((1, 8, 128), jnp.float32)],
    )
    totals = sum(totals_of(sums))
    last_step = totals[0] / (totals[1] + DAMPING * totals[0])
    return object_field + first_step[0] * first_way + last_step * own(middle)


def solution(mesh):
    return jax.shard_map(
        shards,
        mesh=mesh,
        in_specs=(
            P(None, "gx", "gy"),
            P("ma", None, None, None),
            P("gx", "gy", None, None, None),
            P("gx", "gy", None, None),
            P("gx", "gy"),
        ),
        out_specs=P(None, "gx", "gy"),
        check_vma=False,
    )
```

```python
import functools
import math

import jax
import jax.numpy as jnp
import ml_dtypes
import numpy as np
from jax import lax
from jax.experimental import pallas as pl
from jax.experimental.pallas import tpu as pltpu
from jax.sharding import PartitionSpec as P

DAMPING = 1.0
UNROLL = 2
USED, PLACE_MA, SIDE, PLACE_Y, SIDE_Y = range(5)


def dft_tables(width):
    ladder = np.arange(width, dtype=np.int64)
    angles = (ladder[:, None] * ladder[None, :] % width) * (2.0 * math.pi / width)
    real_part = np.cos(angles) / math.sqrt(width)
    imag_part = -np.sin(angles) / math.sqrt(width)
    table_one = np.block([[real_part, -imag_part], [imag_part, real_part]])
    table_two = np.block([[real_part, imag_part], [-imag_part, real_part]])
    return table_one.astype(ml_dtypes.bfloat16), table_two.astype(ml_dtypes.bfloat16)


def pair_swaps(count):
    even = [(i, i ^ 1) for i in range(count) if (i ^ 1) < count]
    if count < 3:
        return [even]
    odd = [(i, i + 1) for i in range(1, count - 1, 2)]
    if count % 2 == 0:
        odd = odd + [(count - 1, 0)]
    return [even, odd + [(target, source) for source, target in odd]]


def side_weights(axis):
    count = lax.axis_size(axis)
    place = lax.axis_index(axis)
    even = place % 2 == 0
    has_low = place > 0
    has_high = place + 1 < count
    flags = [even & has_high, ~even & has_low]
    if count > 2:
        flags = [~even & has_low, even & has_low, even & has_high, ~even & has_high]
    else:
        flags = [~even & has_low, even & has_high]
    return jnp.stack(flags).astype(jnp.float32)


def swap(axis, blocks):
    return [
        lax.ppermute(block, axis, pairs)
        for block, pairs in zip(blocks, pair_swaps(lax.axis_size(axis)))
    ]


def exchanges(count):
    if count & (count - 1):
        return [[(i, (i + k) % count) for i in range(count)] for k in range(1, count)]
    return [[(i, i ^ k) for i in range(count)] for k in range(1, count)]


def source_of(place, k, count):
    if count & (count - 1):
        return lax.rem(place - k + count, count)
    return place ^ k


def dot(left, right):
    return jnp.dot(left, right, preferred_element_type=jnp.float32)


def call(body, name, out_shapes, in_spaces, operands, out_spaces=None, scratch=()):
    specs = [pl.BlockSpec(memory_space=space) for space in in_spaces]
    out_spaces = out_spaces or [pltpu.VMEM] * len(out_shapes)
    operands = [
        pltpu.with_memory_space_constraint(operand, pltpu.VMEM) if space == pltpu.VMEM else operand
        for operand, space in zip(operands, in_spaces)
    ]
    return pl.pallas_call(
        body,
        name=name,
        out_shape=[
            pltpu.VMEM(shape, jnp.float32)
            if space == pltpu.VMEM
            else jax.ShapeDtypeStruct(shape, jnp.float32)
            for shape, space in zip(out_shapes, out_spaces)
        ],
        in_specs=specs,
        out_specs=[pl.BlockSpec(memory_space=space) for space in out_spaces],
        scratch_shapes=list(scratch),
        compiler_params=pltpu.CompilerParams(vmem_limit_bytes=16 * 2**20),
    )(*operands)


class Plan:
    def __init__(self, tile_rows, tile_cols, patch, modes, slots):
        self.tile_rows, self.tile_cols = tile_rows, tile_cols
        self.patch, self.modes, self.slots = patch, modes, slots
        self.rim = patch // 2
        self.rows = tile_rows + patch
        self.cols = tile_cols + patch

    def scratch(self):
        wide = self.patch
        return [
            pltpu.VMEM((2, self.rows, self.cols), jnp.float32),
            pltpu.VMEM((self.slots, 2, wide, wide), jnp.float32),
            pltpu.VMEM((UNROLL, 2 * wide, wide), jnp.bfloat16),
            pltpu.VMEM((UNROLL, 2 * wide, wide), jnp.bfloat16),
        ]

    def fill_region(self, region, middle, received, weights):
        rim, rows = self.rim, self.tile_rows
        count = len(received)
        low = sum(received[k][...] * weights[k] for k in range(count))
        high = sum(received[k][...] * weights[count + k] for k in range(count))
        region[:, :rim] = low
        region[:, rim : rim + rows] = middle[...]
        region[:, rim + rows :] = high

    def row_split(self, row):
        shift = lax.rem(row, 8)
        return pl.multiple_of(row - shift, 8), shift

    def take_windows(self, windows, region, centres):
        wide = self.patch
        for slot in range(self.slots):
            for part in range(2):
                base, shift = self.row_split(centres[slot, 0])
                strip = region[part, pl.ds(base, wide + 8), :]
                strip = pltpu.roll(strip, wide + 8 - shift, 0)[:wide]
                turned = pltpu.roll(strip, self.cols - centres[slot, 1], 1)
                windows[slot, part] = turned[:, :wide]

    def place(self, canvas, slot, part, piece, centres):
        strip = jnp.concatenate([piece, jnp.zeros((self.patch, self.cols - self.patch), jnp.float32)], 1)
        strip = jnp.concatenate([strip, jnp.zeros((8, self.cols), jnp.float32)], 0)
        base, shift = self.row_split(centres[slot, 0])
        turned = pltpu.roll(pltpu.roll(strip, centres[slot, 1], 1), shift, 0)
        canvas[part, pl.ds(base, self.patch + 8), :] += turned

    def each_modes(self, slot, body):
        def step(index, carry):
            body([index * UNROLL + j for j in range(UNROLL)])
            return carry

        lax.fori_loop(0, self.modes // UNROLL, step, 0)

    def spectra(self, slot, modes, probes, windows, wave, half, tables):
        wide = self.patch
        x_real, x_imag = windows[slot, 0], windows[slot, 1]
        for j, mode in enumerate(modes):
            p_real, p_imag = probes[mode, 0], probes[mode, 1]
            wave[j, :wide] = (p_real * x_real - p_imag * x_imag).astype(jnp.bfloat16)
            wave[j, wide:] = (p_real * x_imag + p_imag * x_real).astype(jnp.bfloat16)
        for j in range(len(modes)):
            half[j] = dot(tables[0][...], wave[j]).astype(jnp.bfloat16)
        return [
            dot(half[j, :wide], tables[1][:wide]) + dot(half[j, wide:], tables[1][wide:])
            for j in range(len(modes))
        ]

    def images(self, fields, weight, modes, probes, wave, half, tables):
        wide = self.patch
        for j, field in enumerate(fields):
            half[j, :wide] = (2.0 * field[:, :wide] * weight).astype(jnp.bfloat16)
            half[j, wide:] = (2.0 * field[:, wide:] * weight).astype(jnp.bfloat16)
        for j in range(len(modes)):
            turned = dot(half[j, :wide], tables[0][:wide]) + dot(half[j, wide:], tables[0][wide:])
            turned = turned.astype(jnp.bfloat16)
            wave[j, :wide] = turned[:, :wide]
            wave[j, wide:] = turned[:, wide:]
        real_sum = imag_sum = 0.0
        for j, mode in enumerate(modes):
            back = dot(tables[1][...], wave[j])
            p_real, p_imag = probes[mode, 0], probes[mode, 1]
            real_sum = real_sum + (p_real * back[:wide] + p_imag * back[wide:])
            imag_sum = imag_sum + (p_real * back[wide:] - p_imag * back[:wide])
        return real_sum, imag_sum

    def send(self, canvas, parity, middle_out, sends):
        rim, rows = self.rim, self.tile_rows
        middle_out[...] = canvas[:, rim : rim + rows]
        for k, out in enumerate(sends):
            upper = parity if k == 0 else 1 - parity
            start = pl.multiple_of((1 - upper) * (rim + rows), 8)
            out[...] = canvas[:, pl.ds(start, rim), :]


def start_body(plan, swaps, grid, *refs):
    refs = list(refs)
    info, centres, weights, middle = refs[:4]
    received = refs[4 : 4 + swaps]
    shard, packed, crossed, targets, one, two = refs[4 + swaps : 10 + swaps]
    spectra, intensity, probes, middle_out, *tail = refs[10 + swaps :]
    sends = tail[:swaps]
    region, windows, wave, half, image = tail[swaps:]
    wide = plan.patch
    columns, shards = grid
    lead = plan.modes // shards
    tables = (one, two)
    span = wide // (2 * columns)

    probes[pl.ds(info[PLACE_MA] * lead, lead)] = shard[...]
    for k in range(1, shards):
        home = source_of(info[PLACE_MA], k, shards) * lead
        for c in range(columns):
            column = source_of(info[PLACE_Y], c, columns) * span
            near = pl.multiple_of(info[SIDE] * (wide // 2) + column, 8)
            far = pl.multiple_of((1 - info[SIDE]) * (wide // 2) + column, 8)
            probes[pl.ds(home, lead), :, pl.ds(near, span), :] = packed[k - 1, c]
            probes[pl.ds(home, lead), :, pl.ds(far, span), :] = crossed[k - 1, c]

    plan.fill_region(region, middle, received, weights)
    plan.take_windows(windows, region, centres)
    region[...] = jnp.zeros_like(region)
    for slot in range(plan.slots):
        intensity[slot] = jnp.zeros((wide, wide), jnp.float32)

        def forward(modes):
            fields = plan.spectra(slot, modes, probes, windows, wave, half, tables)
            power = 0.0
            for mode, field in zip(modes, fields):
                spectra[slot * plan.modes + mode] = field
                power = power + (field[:, :wide] * field[:, :wide] + field[:, wide:] * field[:, wide:])
            intensity[slot] += power

        plan.each_modes(slot, forward)
        live = jnp.where(slot < info[USED], 1.0, 0.0)
        windows[slot, 0] = live * (intensity[slot] - targets[slot])
        image[...] = jnp.zeros_like(image)

        def backward(modes):
            fields = [spectra[slot * plan.modes + mode] for mode in modes]
            real_sum, imag_sum = plan.images(fields, windows[slot, 0], modes, probes, wave, half, tables)
            image[0] += real_sum
            image[1] += imag_sum

        plan.each_modes(slot, backward)
        for part in range(2):
            plan.place(region, slot, part, image[part], centres)
    plan.send(region, info[SIDE], middle_out, sends)


def change_body(plan, swaps, last, *refs):
    refs = list(refs)
    info, centres, weights, middle = refs[:4]
    received = refs[4 : 4 + swaps]
    spectra, probes, one, two = refs[4 + swaps : 8 + swaps]
    outs = refs[8 + swaps :]
    if last:
        sums, region, windows, wave, half, change, power = outs
    else:
        sums, moved, change, power, region, windows, wave, half = outs
    wide, rim = plan.patch, plan.rim
    tables = (one, two)
    plan.fill_region(region, middle, received, weights)
    plan.take_windows(windows, region, centres)
    own = middle[:, :, rim : rim + plan.tile_cols]
    sums[0] = jnp.sum(own * own)
    bend = 0.0
    for slot in range(plan.slots):
        change[slot] = jnp.zeros((wide, wide), jnp.float32)
        if not last:
            power[slot] = jnp.zeros((wide, wide), jnp.float32)

        def forward(modes):
            fields = plan.spectra(slot, modes, probes, windows, wave, half, tables)
            cross = square = 0.0
            for mode, field in zip(modes, fields):
                base = spectra[slot * plan.modes + mode]
                cross = cross + (base[:, :wide] * field[:, :wide] + base[:, wide:] * field[:, wide:])
                if not last:
                    moved[slot * plan.modes + mode] = field
                    square = square + (
                        field[:, :wide] * field[:, :wide] + field[:, wide:] * field[:, wide:]
                    )
            change[slot] += 2.0 * cross
            if not last:
                power[slot] += square

        plan.each_modes(slot, forward)
        live = jnp.where(slot < info[USED], 1.0, 0.0)
        bend = bend + live * jnp.sum(change[slot] * change[slot])
    sums[1] = bend


def image_body(plan, swaps, parts, *refs):
    refs = list(refs)
    info, centres = refs[:2]
    totals = refs[2 : 2 + parts]
    spectra, moved, intensity, change, power, probes, targets, one, two = refs[2 + parts : 11 + parts]
    fresh, step_out, middle_out, *tail = refs[11 + parts :]
    sends = tail[:swaps]
    region, windows, wave, half, image = tail[swaps:]
    tables = (one, two)
    step = step_of(totals)
    step_out[0] = step
    region[...] = jnp.zeros_like(region)
    for slot in range(plan.slots):
        live = jnp.where(slot < info[USED], 1.0, 0.0)
        bright = intensity[slot] + step * (change[slot] + step * power[slot])
        windows[slot, 0] = live * (bright - targets[slot])
        image[...] = jnp.zeros_like(image)

        def backward(modes):
            fields = []
            for mode in modes:
                field = spectra[slot * plan.modes + mode] + step * moved[slot * plan.modes + mode]
                fresh[slot * plan.modes + mode] = field
                fields.append(field)
            real_sum, imag_sum = plan.images(fields, windows[slot, 0], modes, probes, wave, half, tables)
            image[0] += real_sum
            image[1] += imag_sum

        plan.each_modes(slot, backward)
        for part in range(2):
            plan.place(region, slot, part, image[part], centres)
    plan.send(region, info[SIDE], middle_out, sends)


def step_of(totals):
    values = [[part[k] for part in totals] for k in range(2)]
    while len(values[0]) > 1:
        values = [[v[i] + v[i + 1] for i in range(0, len(v), 2)] for v in values]
    norm, bend = values[0][0], values[1][0]
    top = jnp.full((8, 128), norm, jnp.float32)
    return jnp.max(top / (bend + DAMPING * norm))


def pack_body(plan, swaps, columns, *refs):
    info, shard, tile, mine, *rims = refs
    span = plan.patch // (2 * columns)
    start = pl.multiple_of(info[SIDE] * (plan.patch // 2) + info[PLACE_Y] * span, 8)
    mine[...] = shard[:, :, pl.ds(start, span), :]
    low, high = tile[:, :, : plan.rim], tile[:, :, plan.tile_cols - plan.rim :]
    for k, rim in enumerate(rims):
        rim[...] = jnp.where((info[SIDE_Y] == 0) == (k == 0), high, low)


def join_body(plan, swaps, columns, shards, *refs):
    weights, tile = refs[:2]
    received = refs[2 : 2 + swaps]
    parts = refs[2 + swaps : -2]
    middle, packed = refs[-2:]
    low, high = sides_of(received, weights)
    middle[:, :, : plan.rim] = low
    middle[:, :, plan.rim : plan.rim + plan.tile_cols] = tile[...]
    middle[:, :, plan.rim + plan.tile_cols :] = high
    for k in range(shards - 1):
        for c in range(columns):
            packed[k, c] = parts[k * columns + c][...]


def sides_of(received, weights):
    count = len(received)
    low = sum(received[k][...] * weights[k] for k in range(count))
    high = sum(received[k][...] * weights[count + k] for k in range(count))
    return low, high


def fold_body(plan, swaps, *refs):
    info, weights, middle = refs[:3]
    received = refs[3 : 3 + swaps]
    merged, *sends = refs[3 + swaps :]
    low, high = sides_of(received, weights)
    merged[...] = middle[...]
    merged[:, : plan.rim] += low
    merged[:, plan.tile_rows - plan.rim :] += high
    for k, out in enumerate(sends):
        left, right = merged[:, :, : plan.patch], merged[:, :, plan.tile_cols :]
        out[...] = jnp.where((info[SIDE_Y] == 0) == (k == 0), right, left)


def halo_body(plan, swaps, *refs):
    weights, inside, merged = refs[:3]
    received = refs[3 : 3 + swaps]
    (middle,) = refs[3 + swaps :]
    low, high = sides_of(received, weights)
    middle[...] = -merged[...]
    middle[:, :, : plan.patch] -= low
    middle[:, :, plan.tile_cols :] -= high
    middle[:, :, : plan.rim] *= inside[0]
    middle[:, :, plan.rim + plan.tile_cols :] *= inside[1]


def finish_body(plan, parts, *refs):
    totals = refs[:parts]
    first_step, tile, first, last, out = refs[parts:]
    span = pl.ds(plan.rim, plan.tile_cols)
    out[...] = tile[...] + first_step[0] * first[:, :, span] + step_of(totals) * last[:, :, span]


def totals_of(sums):
    if lax.axis_size("gx") == 2:
        sums = sums + swap("gx", [sums])[0]
    else:
        sums = lax.psum(sums, "gx")
    count = lax.axis_size("gy")
    if count & (count - 1):
        return [lax.psum(sums, "gy")]
    return [sums] + [lax.ppermute(sums, "gy", pairs) for pairs in exchanges(count)]


def shards(object_field, probe_shard, measured, positions, slot_counts):
    patch = probe_shard.shape[-1]
    tile_rows, tile_cols = object_field.shape[1:]
    columns, groups = lax.axis_size("gy"), lax.axis_size("ma")
    lead = probe_shard.shape[0]
    modes = lead * groups
    slots = measured.shape[2]
    plan = Plan(tile_rows, tile_cols, patch, modes, slots)
    rim, units = plan.rim, slots * modes
    one, two = (jnp.asarray(table) for table in dft_tables(patch))
    targets = measured[0, 0]
    centres = positions[0, 0]
    gx, gy, ma = (lax.axis_index(axis) for axis in ("gx", "gy", "ma"))
    info = jnp.stack([slot_counts[0, 0], ma, gx % 2, gy, gy % 2])
    weights_x, weights_y = side_weights("gx"), side_weights("gy")
    inside = jnp.stack([gy > 0, gy + 1 < columns]).astype(jnp.float32)
    info, centres, weights_x, weights_y, inside = lax.optimization_barrier(
        (info, centres, weights_x, weights_y, inside)
    )
    swaps_x, swaps_y = (len(pair_swaps(lax.axis_size(axis))) for axis in ("gx", "gy"))
    smem, vmem = pltpu.SMEM, pltpu.VMEM
    tall = (2, tile_rows, plan.cols)
    fold = (2, rim, plan.cols)
    image_scratch = pltpu.VMEM((2, patch, patch), jnp.float32)
    span = patch // (2 * columns)

    def rows_around(middle):
        if rim == tile_rows:
            return swap("gx", [middle] * swaps_x)
        even = gx % 2 == 0
        ends = [middle[:, :rim], middle[:, tile_rows - rim :]]
        blocks = [jnp.where(even, ends[1], ends[0]), jnp.where(even, ends[0], ends[1])]
        return swap("gx", blocks[:swaps_x])

    def descent(middle, sends):
        merged, *blocks = call(
            functools.partial(fold_body, plan, swaps_x),
            "fold",
            [tall] + [(2, tile_rows, patch)] * swaps_y,
            [smem] * 2 + [vmem] * (1 + swaps_x),
            [info, weights_x, middle, *swap("gx", sends)],
        )
        (middle,) = call(
            functools.partial(halo_body, plan, swaps_y),
            "halo",
            [tall],
            [smem] * 2 + [vmem] * (1 + swaps_y),
            [weights_y, inside, merged, *swap("gy", blocks)],
        )
        return middle

    mine, *rims = call(
        functools.partial(pack_body, plan, swaps_y, columns),
        "pack",
        [(lead, 2, span, patch)] + [(2, tile_rows, rim)] * swaps_y,
        [smem] + [vmem] * 2,
        [info, probe_shard, object_field],
    )
    parts = []
    for pairs in exchanges(groups):
        block = lax.ppermute(mine, "ma", pairs)
        parts += [block] + [lax.ppermute(block, "gy", others) for others in exchanges(columns)]
    middle, packed = call(
        functools.partial(join_body, plan, swaps_y, columns, groups),
        "join",
        [tall, (groups - 1, columns, lead, 2, span, patch)],
        [smem] + [vmem] * (1 + swaps_y + len(parts)),
        [weights_y, object_field, *swap("gy", rims), *parts],
    )
    (crossed,) = swap("gx", [packed])[:1]

    spectra, intensity, probes, middle, *sends = call(
        functools.partial(start_body, plan, swaps_x, (columns, groups)),
        "start",
        [(units, patch, 2 * patch), (slots, patch, patch), (modes, 2, patch, patch), tall]
        + [fold] * swaps_x,
        [smem] * 3 + [vmem] * (7 + swaps_x),
        [info, centres, weights_x, middle, *rows_around(middle), probe_shard, packed, crossed]
        + [targets, one, two],
        scratch=plan.scratch() + [image_scratch],
    )
    first_way = descent(middle, sends)
    sums, moved, change, power = call(
        functools.partial(change_body, plan, swaps_x, False),
        "change",
        [(2,), (units, patch, 2 * patch), (slots, patch, patch), (slots, patch, patch)],
        [smem] * 3 + [vmem] * (5 + swaps_x),
        [info, centres, weights_x, first_way, *rows_around(first_way), spectra, probes, one, two],
        [smem] + [vmem] * 3,
        scratch=plan.scratch(),
    )
    totals = totals_of(sums)
    spectra, first_step, middle, *sends = call(
        functools.partial(image_body, plan, swaps_x, len(totals)),
        "image",
        [(units, patch, 2 * patch), (1,), tall] + [fold] * swaps_x,
        [smem] * (2 + len(totals)) + [vmem] * 9,
        [info, centres, *totals, spectra, moved, intensity, change, power, probes, targets, one, two],
        [vmem, smem] + [vmem] * (1 + swaps_x),
        scratch=plan.scratch() + [image_scratch],
    )
    last_way = descent(middle, sends)
    (sums,) = call(
        functools.partial(change_body, plan, swaps_x, True),
        "last_change",
        [(2,)],
        [smem] * 3 + [vmem] * (5 + swaps_x),
        [info, centres, weights_x, last_way, *rows_around(last_way), spectra, probes, one, two],
        [smem],
        scratch=plan.scratch()
        + [pltpu.VMEM((slots, patch, patch), jnp.float32), pltpu.VMEM((1, 8, 128), jnp.float32)],
    )
    totals = totals_of(sums)
    (current,) = call(
        functools.partial(finish_body, plan, len(totals)),
        "finish",
        [(2, tile_rows, tile_cols)],
        [smem] * (len(totals) + 1) + [vmem] * 3,
        [*totals, first_step, object_field, first_way, last_way],
    )
    return current


def solution(mesh):
    return jax.shard_map(
        shards,
        mesh=mesh,
        in_specs=(
            P(None, "gx", "gy"),
            P("ma", None, None, None),
            P("gx", "gy", None, None, None),
            P("gx", "gy", None, None),
            P("gx", "gy"),
        ),
        out_specs=P(None, "gx", "gy"),
        check_vma=False,
    )
```

```python
import functools
import math

import jax
import jax.numpy as jnp
import ml_dtypes
import numpy as np
from jax import lax
from jax.experimental import pallas as pl
from jax.experimental.pallas import tpu as pltpu
from jax.sharding import PartitionSpec as P

DAMPING = 1.0
UNROLL = 2
USED, PLACE_MA, SIDE, PLACE_Y, SIDE_Y = range(5)


def dft_tables(width):
    ladder = np.arange(width, dtype=np.int64)
    angles = (ladder[:, None] * ladder[None, : width // 2] % width) * (2.0 * math.pi / width)
    real_part = np.cos(angles) / math.sqrt(width)
    imag_part = -np.sin(angles) / math.sqrt(width)
    blocks = [
        np.block([[real_part[p::2], -imag_part[p::2]], [imag_part[p::2], real_part[p::2]]])
        for p in range(2)
    ]
    one = np.stack(blocks).astype(ml_dtypes.bfloat16)
    return one, np.ascontiguousarray(one.transpose(0, 2, 1))


def pair_swaps(count):
    even = [(i, i ^ 1) for i in range(count) if (i ^ 1) < count]
    if count < 3:
        return [even]
    odd = [(i, i + 1) for i in range(1, count - 1, 2)]
    if count % 2 == 0:
        odd = odd + [(count - 1, 0)]
    return [even, odd + [(target, source) for source, target in odd]]


def side_weights(axis):
    count = lax.axis_size(axis)
    place = lax.axis_index(axis)
    even = place % 2 == 0
    has_low = place > 0
    has_high = place + 1 < count
    flags = [even & has_high, ~even & has_low]
    if count > 2:
        flags = [~even & has_low, even & has_low, even & has_high, ~even & has_high]
    else:
        flags = [~even & has_low, even & has_high]
    return jnp.stack(flags).astype(jnp.float32)


def swap(axis, blocks):
    return [
        lax.ppermute(block, axis, pairs)
        for block, pairs in zip(blocks, pair_swaps(lax.axis_size(axis)))
    ]


def exchanges(count):
    if count & (count - 1):
        return [[(i, (i + k) % count) for i in range(count)] for k in range(1, count)]
    return [[(i, i ^ k) for i in range(count)] for k in range(1, count)]


def source_of(place, k, count):
    if count & (count - 1):
        return lax.rem(place - k + count, count)
    return place ^ k


def dot(left, right):
    return jnp.dot(left, right, preferred_element_type=jnp.float32)


def call(body, name, out_shapes, in_spaces, operands, out_spaces=None, scratch=(), pinned=True, dtypes={}):
    specs = [pl.BlockSpec(memory_space=space) for space in in_spaces]
    out_spaces = out_spaces or [pltpu.VMEM] * len(out_shapes)
    operands = [
        pltpu.with_memory_space_constraint(operand, pltpu.VMEM) if pinned and space == pltpu.VMEM else operand
        for operand, space in zip(operands, in_spaces)
    ]
    return pl.pallas_call(
        body,
        name=name,
        out_shape=[
            space(shape, dtypes.get(k, jnp.float32))
            if space == pltpu.VMEM
            else jax.ShapeDtypeStruct(shape, jnp.float32)
            for k, (shape, space) in enumerate(zip(out_shapes, out_spaces))
        ],
        in_specs=specs,
        out_specs=[pl.BlockSpec(memory_space=space or pltpu.VMEM) for space in out_spaces],
        scratch_shapes=list(scratch),
        compiler_params=pltpu.CompilerParams(vmem_limit_bytes=16 * 2**20),
    )(*operands)


class Plan:
    def __init__(self, tile_rows, tile_cols, patch, modes, slots):
        self.tile_rows, self.tile_cols = tile_rows, tile_cols
        self.patch, self.modes, self.slots = patch, modes, slots
        self.rim = patch // 2
        self.rows = tile_rows + patch
        self.cols = tile_cols + patch

    def scratch(self):
        wide = self.patch
        return [
            pltpu.VMEM((2, self.rows, self.cols), jnp.float32),
            pltpu.VMEM((self.slots, 2, wide, wide), jnp.float32),
            pltpu.VMEM((UNROLL, 2, wide, wide), jnp.bfloat16),
            pltpu.VMEM((UNROLL, 2, wide, wide), jnp.bfloat16),
        ]

    def fill_region(self, region, middle, received, weights):
        rim, rows = self.rim, self.tile_rows
        count = len(received)
        low = sum(received[k][...] * weights[k] for k in range(count))
        high = sum(received[k][...] * weights[count + k] for k in range(count))
        region[:, :rim] = low
        region[:, rim : rim + rows] = middle[...]
        region[:, rim + rows :] = high

    def row_split(self, row):
        shift = lax.rem(row, 8)
        return pl.multiple_of(row - shift, 8), shift

    def take_windows(self, windows, region, centres):
        wide = self.patch
        for slot in range(self.slots):
            for part in range(2):
                base, shift = self.row_split(centres[slot, 0])
                strip = region[part, pl.ds(base, wide + 8), :]
                strip = pltpu.roll(strip, wide + 8 - shift, 0)[:wide]
                turned = pltpu.roll(strip, self.cols - centres[slot, 1], 1)
                windows[slot, part] = turned[:, :wide]

    def place(self, canvas, slot, part, piece, centres):
        strip = jnp.concatenate([piece, jnp.zeros((self.patch, self.cols - self.patch), jnp.float32)], 1)
        strip = jnp.concatenate([strip, jnp.zeros((8, self.cols), jnp.float32)], 0)
        base, shift = self.row_split(centres[slot, 0])
        turned = pltpu.roll(pltpu.roll(strip, centres[slot, 1], 1), shift, 0)
        canvas[part, pl.ds(base, self.patch + 8), :] += turned

    def each_modes(self, slot, body):
        def step(index, carry):
            body([index * UNROLL + j for j in range(UNROLL)])
            return carry

        lax.fori_loop(0, self.modes // UNROLL, step, 0)

    def spectra(self, slot, modes, probes, windows, wave, half, tables):
        mid = self.rim
        low, high = slice(0, mid), slice(mid, 2 * mid)
        for j, mode in enumerate(modes):
            ends = []
            for rows in (low, high):
                p_real, p_imag = probes[mode, 0, rows], probes[mode, 1, rows]
                x_real, x_imag = windows[slot, 0, rows], windows[slot, 1, rows]
                ends.append((p_real * x_real - p_imag * x_imag, p_real * x_imag + p_imag * x_real))
            for part, rows in enumerate((low, high)):
                wave[j, 0, rows] = (ends[0][part] + ends[1][part]).astype(jnp.bfloat16)
                wave[j, 1, rows] = (ends[0][part] - ends[1][part]).astype(jnp.bfloat16)
        for j in range(len(modes)):
            for k, rows in enumerate((low, high)):
                strip = dot(tables[0][k], wave[j, k])
                for part, source in enumerate((low, high)):
                    left, right = strip[source, low], strip[source, high]
                    target = slice(part * mid, (part + 1) * mid)
                    half[j, 0, rows, target] = (left + right).astype(jnp.bfloat16)
                    half[j, 1, rows, target] = (left - right).astype(jnp.bfloat16)
        return [[dot(half[j, k], tables[1][k]) for k in range(2)] for j in range(len(modes))]

    def paired(self, first, second):
        mid = self.rim
        products = [a * b for a, b in zip(first, second)]
        return jnp.concatenate([p[:, :mid] + p[:, mid:] for p in products], 1)

    def load(self, spectra, unit):
        wide = self.patch
        return [spectra[unit, :, :wide], spectra[unit, :, wide:]]

    def store(self, spectra, unit, field):
        wide = self.patch
        spectra[unit, :, :wide], spectra[unit, :, wide:] = field

    def images(self, fields, weight, modes, probes, wave, half, tables):
        mid = self.rim
        low, high = slice(0, mid), slice(mid, 2 * mid)
        doubled = 2.0 * weight
        for j, field in enumerate(fields):
            for k, columns in enumerate((low, high)):
                factor = jnp.concatenate([doubled[:, columns]] * 2, 1)
                half[j, k] = (field[k] * factor).astype(jnp.bfloat16)
        for j in range(len(modes)):
            even, odd = (dot(half[j, k], tables[0][k]) for k in range(2))
            for columns, turned in ((low, even + odd), (high, even - odd)):
                turned = turned.astype(jnp.bfloat16)
                for k, rows in enumerate((low, high)):
                    wave[j, k, low, columns] = turned[rows, low]
                    wave[j, k, high, columns] = turned[rows, high]
        sums = [[0.0, 0.0], [0.0, 0.0]]
        for j, mode in enumerate(modes):
            even, odd = (dot(tables[1][k], wave[j, k]) for k in range(2))
            for side, (rows, back) in enumerate(((low, even + odd), (high, even - odd))):
                p_real, p_imag = probes[mode, 0, rows], probes[mode, 1, rows]
                sums[side][0] = sums[side][0] + (p_real * back[low] + p_imag * back[high])
                sums[side][1] = sums[side][1] + (p_real * back[high] - p_imag * back[low])
        return sums

    def add_images(self, image, sums):
        mid = self.rim
        for side in range(2):
            for part in range(2):
                image[part, side * mid : (side + 1) * mid] += sums[side][part]

    def send(self, canvas, parity, middle_out, sends):
        rim, rows = self.rim, self.tile_rows
        middle_out[...] = canvas[:, rim : rim + rows]
        for k, out in enumerate(sends):
            upper = parity if k == 0 else 1 - parity
            start = pl.multiple_of((1 - upper) * (rim + rows), 8)
            out[...] = canvas[:, pl.ds(start, rim), :]


def start_body(plan, swaps, grid, *refs):
    refs = list(refs)
    info, centres, weights, middle = refs[:4]
    received = refs[4 : 4 + swaps]
    shard, packed, crossed, targets, one, two = refs[4 + swaps : 10 + swaps]
    spectra, intensity, probes, middle_out, *tail = refs[10 + swaps :]
    sends = tail[:swaps]
    region, windows, wave, half, image = tail[swaps:]
    wide = plan.patch
    columns, shards = grid
    lead = plan.modes // shards
    tables = (one, two)
    span = wide // (2 * columns)

    probes[pl.ds(info[PLACE_MA] * lead, lead)] = shard[...]
    for k in range(1, shards):
        home = source_of(info[PLACE_MA], k, shards) * lead
        for c in range(columns):
            column = source_of(info[PLACE_Y], c, columns) * span
            near = pl.multiple_of(info[SIDE] * (wide // 2) + column, 8)
            far = pl.multiple_of((1 - info[SIDE]) * (wide // 2) + column, 8)
            probes[pl.ds(home, lead), :, pl.ds(near, span), :] = packed[k - 1, c]
            probes[pl.ds(home, lead), :, pl.ds(far, span), :] = crossed[k - 1, c]

    plan.fill_region(region, middle, received, weights)
    plan.take_windows(windows, region, centres)
    region[...] = jnp.zeros_like(region)
    for slot in range(plan.slots):
        intensity[slot] = jnp.zeros((wide, wide), jnp.float32)

        def forward(modes):
            fields = plan.spectra(slot, modes, probes, windows, wave, half, tables)
            power = 0.0
            for mode, field in zip(modes, fields):
                plan.store(spectra, slot * plan.modes + mode, field)
                power = power + plan.paired(field, field)
            intensity[slot] += power

        plan.each_modes(slot, forward)
        live = jnp.where(slot < info[USED], 1.0, 0.0)
        windows[slot, 0] = live * (intensity[slot] - targets[slot])
        image[...] = jnp.zeros_like(image)

        def backward(modes):
            fields = [plan.load(spectra, slot * plan.modes + mode) for mode in modes]
            sums = plan.images(fields, windows[slot, 0], modes, probes, wave, half, tables)
            plan.add_images(image, sums)

        plan.each_modes(slot, backward)
        for part in range(2):
            plan.place(region, slot, part, image[part], centres)
    plan.send(region, info[SIDE], middle_out, sends)


def change_body(plan, swaps, last, *refs):
    refs = list(refs)
    info, centres, weights, middle = refs[:4]
    received = refs[4 : 4 + swaps]
    spectra, probes, one, two = refs[4 + swaps : 8 + swaps]
    outs = refs[8 + swaps :]
    if last:
        sums, region, windows, wave, half, change, power = outs
    else:
        sums, moved, change, power, region, windows, wave, half = outs
    wide, rim = plan.patch, plan.rim
    tables = (one, two)
    plan.fill_region(region, middle, received, weights)
    plan.take_windows(windows, region, centres)
    own = middle[:, :, rim : rim + plan.tile_cols]
    sums[0] = jnp.sum(own * own)
    bend = 0.0
    for slot in range(plan.slots):
        change[slot] = jnp.zeros((wide, wide), jnp.float32)
        if not last:
            power[slot] = jnp.zeros((wide, wide), jnp.float32)

        def forward(modes):
            fields = plan.spectra(slot, modes, probes, windows, wave, half, tables)
            cross = square = 0.0
            for mode, field in zip(modes, fields):
                cross = cross + plan.paired(plan.load(spectra, slot * plan.modes + mode), field)
                if not last:
                    plan.store(moved, slot * plan.modes + mode, field)
                    square = square + plan.paired(field, field)
            change[slot] += 2.0 * cross
            if not last:
                power[slot] += square

        plan.each_modes(slot, forward)
        live = jnp.where(slot < info[USED], 1.0, 0.0)
        bend = bend + live * jnp.sum(change[slot] * change[slot])
    sums[1] = bend


def image_body(plan, swaps, parts, *refs):
    refs = list(refs)
    info, centres = refs[:2]
    totals = refs[2 : 2 + parts]
    spectra, moved, intensity, change, power, probes, targets, one, two = refs[2 + parts : 11 + parts]
    fresh, step_out, middle_out, *tail = refs[11 + parts :]
    sends = tail[:swaps]
    region, windows, wave, half, image = tail[swaps:]
    tables = (one, two)
    step = step_of(totals)
    step_out[0] = step
    region[...] = jnp.zeros_like(region)
    for slot in range(plan.slots):
        live = jnp.where(slot < info[USED], 1.0, 0.0)
        bright = intensity[slot] + step * (change[slot] + step * power[slot])
        windows[slot, 0] = live * (bright - targets[slot])
        image[...] = jnp.zeros_like(image)

        def backward(modes):
            fields = []
            for mode in modes:
                unit = slot * plan.modes + mode
                pairs = zip(plan.load(spectra, unit), plan.load(moved, unit))
                fields.append([base + step * shift for base, shift in pairs])
                plan.store(fresh, unit, fields[-1])
            sums = plan.images(fields, windows[slot, 0], modes, probes, wave, half, tables)
            plan.add_images(image, sums)

        plan.each_modes(slot, backward)
        for part in range(2):
            plan.place(region, slot, part, image[part], centres)
    plan.send(region, info[SIDE], middle_out, sends)


def step_of(totals):
    values = [[part[k] for part in totals] for k in range(2)]
    while len(values[0]) > 1:
        values = [[v[i] + v[i + 1] for i in range(0, len(v), 2)] for v in values]
    norm, bend = values[0][0], values[1][0]
    top = jnp.full((8, 128), norm, jnp.float32)
    return jnp.max(top / (bend + DAMPING * norm))


def pack_body(plan, swaps, columns, *refs):
    info, shard, tile, mine, *rims = refs
    span = plan.patch // (2 * columns)
    start = pl.multiple_of(info[SIDE] * (plan.patch // 2) + info[PLACE_Y] * span, 8)
    mine[...] = shard[:, :, pl.ds(start, span), :]
    low, high = tile[:, :, : plan.rim], tile[:, :, plan.tile_cols - plan.rim :]
    for k, rim in enumerate(rims):
        rim[...] = jnp.where((info[SIDE_Y] == 0) == (k == 0), high, low)


def stage_body(plan, *refs):
    targets, one, two, shard, _, ordered, *copies = refs
    wide = plan.patch
    place = lax.broadcasted_iota(jnp.int32, (wide, wide), 0)
    source = jnp.where(place < plan.rim, 2 * place, 2 * (place - plan.rim) + 1)
    pick = jnp.where(source == lax.broadcasted_iota(jnp.int32, (wide, wide), 1), 1.0, 0.0)
    pick = pick.astype(jnp.bfloat16)

    def parts_of(block):
        parts = []
        for _ in range(3):
            parts.append(block.astype(jnp.bfloat16))
            block = block - parts[-1].astype(jnp.float32)
        return parts

    for slot in range(plan.slots):
        rows = sum(dot(pick, part) for part in parts_of(targets[slot]))
        ordered[slot] = sum(
            lax.dot_general(part, pick, (((1,), (1,)), ((), ())), preferred_element_type=jnp.float32)
            for part in parts_of(rows)
        )
    for source, copy in zip((one, two, shard), copies):
        copy[...] = source[...]


def join_body(plan, swaps, columns, shards, *refs):
    weights, tile = refs[:2]
    received = refs[2 : 2 + swaps]
    parts = refs[2 + swaps : -2]
    middle, packed = refs[-2:]
    low, high = sides_of(received, weights)
    middle[:, :, : plan.rim] = low
    middle[:, :, plan.rim : plan.rim + plan.tile_cols] = tile[...]
    middle[:, :, plan.rim + plan.tile_cols :] = high
    for k in range(shards - 1):
        for c in range(columns):
            packed[k, c] = parts[k * columns + c][...]


def sides_of(received, weights):
    count = len(received)
    low = sum(received[k][...] * weights[k] for k in range(count))
    high = sum(received[k][...] * weights[count + k] for k in range(count))
    return low, high


def fold_body(plan, swaps, *refs):
    info, weights, middle = refs[:3]
    received = refs[3 : 3 + swaps]
    merged, *sends = refs[3 + swaps :]
    low, high = sides_of(received, weights)
    merged[...] = middle[...]
    merged[:, : plan.rim] += low
    merged[:, plan.tile_rows - plan.rim :] += high
    for k, out in enumerate(sends):
        left, right = merged[:, :, : plan.patch], merged[:, :, plan.tile_cols :]
        out[...] = jnp.where((info[SIDE_Y] == 0) == (k == 0), right, left)


def halo_body(plan, swaps, *refs):
    weights, inside, merged = refs[:3]
    received = refs[3 : 3 + swaps]
    (middle,) = refs[3 + swaps :]
    low, high = sides_of(received, weights)
    middle[...] = -merged[...]
    middle[:, :, : plan.patch] -= low
    middle[:, :, plan.tile_cols :] -= high
    middle[:, :, : plan.rim] *= inside[0]
    middle[:, :, plan.rim + plan.tile_cols :] *= inside[1]


def finish_body(plan, parts, *refs):
    totals = refs[:parts]
    first_step, tile, first, last, out = refs[parts:]
    span = pl.ds(plan.rim, plan.tile_cols)
    out[...] = tile[...] + first_step[0] * first[:, :, span] + step_of(totals) * last[:, :, span]


def totals_of(sums):
    if lax.axis_size("gx") == 2:
        sums = sums + swap("gx", [sums])[0]
    else:
        sums = lax.psum(sums, "gx")
    count = lax.axis_size("gy")
    if count & (count - 1):
        return [lax.psum(sums, "gy")]
    return [sums] + [lax.ppermute(sums, "gy", pairs) for pairs in exchanges(count)]


def shards(object_field, probe_shard, measured, positions, slot_counts):
    patch = probe_shard.shape[-1]
    tile_rows, tile_cols = object_field.shape[1:]
    columns, groups = lax.axis_size("gy"), lax.axis_size("ma")
    lead = probe_shard.shape[0]
    modes = lead * groups
    slots = measured.shape[2]
    plan = Plan(tile_rows, tile_cols, patch, modes, slots)
    rim, units = plan.rim, slots * modes
    one, two = (jnp.asarray(table) for table in dft_tables(patch))
    targets = measured[0, 0]
    centres = positions[0, 0]
    gx, gy, ma = (lax.axis_index(axis) for axis in ("gx", "gy", "ma"))
    info = jnp.stack([slot_counts[0, 0], ma, gx % 2, gy, gy % 2])
    weights_x, weights_y = side_weights("gx"), side_weights("gy")
    inside = jnp.stack([gy > 0, gy + 1 < columns]).astype(jnp.float32)
    info, centres, weights_x, weights_y, inside = lax.optimization_barrier(
        (info, centres, weights_x, weights_y, inside)
    )
    swaps_x, swaps_y = (len(pair_swaps(lax.axis_size(axis))) for axis in ("gx", "gy"))
    smem, vmem = pltpu.SMEM, pltpu.VMEM
    tall = (2, tile_rows, plan.cols)
    fold = (2, rim, plan.cols)
    image_scratch = pltpu.VMEM((2, patch, patch), jnp.float32)
    span = patch // (2 * columns)

    def rows_around(middle):
        if rim == tile_rows:
            return swap("gx", [middle] * swaps_x)
        even = gx % 2 == 0
        ends = [middle[:, :rim], middle[:, tile_rows - rim :]]
        blocks = [jnp.where(even, ends[1], ends[0]), jnp.where(even, ends[0], ends[1])]
        return swap("gx", blocks[:swaps_x])

    def descent(middle, sends):
        merged, *blocks = call(
            functools.partial(fold_body, plan, swaps_x),
            "fold",
            [tall] + [(2, tile_rows, patch)] * swaps_y,
            [smem] * 2 + [vmem] * (1 + swaps_x),
            [info, weights_x, middle, *swap("gx", sends)],
        )
        (middle,) = call(
            functools.partial(halo_body, plan, swaps_y),
            "halo",
            [tall],
            [smem] * 2 + [vmem] * (1 + swaps_y),
            [weights_y, inside, merged, *swap("gy", blocks)],
        )
        return middle

    mine, *rims = call(
        functools.partial(pack_body, plan, swaps_y, columns),
        "pack",
        [(lead, 2, span, patch)] + [(2, tile_rows, rim)] * swaps_y,
        [smem] + [vmem] * 2,
        [info, probe_shard, object_field],
        pinned=False,
    )
    targets, one, two, own_shard = call(
        functools.partial(stage_body, plan),
        "stage",
        [targets.shape, one.shape, two.shape, probe_shard.shape],
        [vmem] * 4 + [pl.ANY],
        [targets, one, two, probe_shard, mine],
        pinned=False,
        dtypes={1: jnp.bfloat16, 2: jnp.bfloat16},
    )
    parts = []
    for pairs in exchanges(groups):
        block = lax.ppermute(mine, "ma", pairs)
        parts += [block] + [lax.ppermute(block, "gy", others) for others in exchanges(columns)]
    middle, packed = call(
        functools.partial(join_body, plan, swaps_y, columns, groups),
        "join",
        [tall, (groups - 1, columns, lead, 2, span, patch)],
        [smem] + [vmem] * (1 + swaps_y + len(parts)),
        [weights_y, object_field, *swap("gy", rims), *parts],
    )
    (crossed,) = swap("gx", [packed])[:1]

    spectra, intensity, probes, middle, *sends = call(
        functools.partial(start_body, plan, swaps_x, (columns, groups)),
        "start",
        [(units, patch, 2 * patch), (slots, patch, patch), (modes, 2, patch, patch), tall]
        + [fold] * swaps_x,
        [smem] * 3 + [vmem] * (7 + swaps_x),
        [info, centres, weights_x, middle, *rows_around(middle), own_shard, packed, crossed]
        + [targets, one, two],
        scratch=plan.scratch() + [image_scratch],
    )
    first_way = descent(middle, sends)
    sums, moved, change, power = call(
        functools.partial(change_body, plan, swaps_x, False),
        "change",
        [(2,), (units, patch, 2 * patch), (slots, patch, patch), (slots, patch, patch)],
        [smem] * 3 + [vmem] * (5 + swaps_x),
        [info, centres, weights_x, first_way, *rows_around(first_way), spectra, probes, one, two],
        [smem] + [vmem] * 3,
        scratch=plan.scratch(),
    )
    totals = totals_of(sums)
    spectra, first_step, middle, *sends = call(
        functools.partial(image_body, plan, swaps_x, len(totals)),
        "image",
        [(units, patch, 2 * patch), (1,), tall] + [fold] * swaps_x,
        [smem] * (2 + len(totals)) + [vmem] * 9,
        [info, centres, *totals, spectra, moved, intensity, change, power, probes, targets, one, two],
        [vmem, smem] + [vmem] * (1 + swaps_x),
        scratch=plan.scratch() + [image_scratch],
    )
    last_way = descent(middle, sends)
    (sums,) = call(
        functools.partial(change_body, plan, swaps_x, True),
        "last_change",
        [(2,)],
        [smem] * 3 + [vmem] * (5 + swaps_x),
        [info, centres, weights_x, last_way, *rows_around(last_way), spectra, probes, one, two],
        [smem],
        scratch=plan.scratch()
        + [pltpu.VMEM((slots, patch, patch), jnp.float32), pltpu.VMEM((1, 8, 128), jnp.float32)],
    )
    totals = totals_of(sums)
    (current,) = call(
        functools.partial(finish_body, plan, len(totals)),
        "finish",
        [(2, tile_rows, tile_cols)],
        [smem] * (len(totals) + 1) + [vmem] * 3,
        [*totals, first_step, object_field, first_way, last_way],
        [None],
    )
    return current


def solution(mesh):
    return jax.shard_map(
        shards,
        mesh=mesh,
        in_specs=(
            P(None, "gx", "gy"),
            P("ma", None, None, None),
            P("gx", "gy", None, None, None),
            P("gx", "gy", None, None),
            P("gx", "gy"),
        ),
        out_specs=P(None, "gx", "gy"),
        check_vma=False,
    )
```

```python
import functools
import math

import jax
import jax.numpy as jnp
import ml_dtypes
import numpy as np
from jax import lax
from jax.experimental import pallas as pl
from jax.experimental.pallas import tpu as pltpu
from jax.sharding import PartitionSpec as P


DAMPING = 1.0
UNROLL = 2
BROAD = 2
USED, PLACE_MA, SIDE, PLACE_Y, SIDE_Y = range(5)


def dft_tables(width):
    ladder = np.arange(width, dtype=np.int64)
    angles = (ladder[:, None] * ladder[None, : width // 2] % width) * (2.0 * math.pi / width)
    real_part = np.cos(angles) / math.sqrt(width)
    imag_part = -np.sin(angles) / math.sqrt(width)
    blocks = [
        np.block([[real_part[p::2], -imag_part[p::2]], [imag_part[p::2], real_part[p::2]]])
        for p in range(2)
    ]
    one = np.stack(blocks).astype(ml_dtypes.bfloat16)
    return one, np.ascontiguousarray(one.transpose(0, 2, 1))


def pair_swaps(count):
    even = [(i, i ^ 1) for i in range(count) if (i ^ 1) < count]
    if count < 3:
        return [even]
    odd = [(i, i + 1) for i in range(1, count - 1, 2)]
    if count % 2 == 0:
        odd = odd + [(count - 1, 0)]
    return [even, odd + [(target, source) for source, target in odd]]


def side_weights(axis):
    count = lax.axis_size(axis)
    place = lax.axis_index(axis)
    even = place % 2 == 0
    has_low = place > 0
    has_high = place + 1 < count
    flags = [even & has_high, ~even & has_low]
    if count > 2:
        flags = [~even & has_low, even & has_low, even & has_high, ~even & has_high]
    else:
        flags = [~even & has_low, even & has_high]
    return jnp.stack(flags).astype(jnp.float32)


def swap(axis, blocks):
    return [lax.ppermute(block, axis, pairs) for block, pairs in zip(blocks, pair_swaps(lax.axis_size(axis)))]


def exchanges(count):
    if count & (count - 1):
        return [[(i, (i + k) % count) for i in range(count)] for k in range(1, count)]
    return [[(i, i ^ k) for i in range(count)] for k in range(1, count)]


def source_of(place, k, count):
    if count & (count - 1):
        return lax.rem(place - k + count, count)
    return place ^ k


def dot(left, right):
    return jnp.dot(left, right, preferred_element_type=jnp.float32)


def call(body, out_shapes, in_spaces, operands, out_spaces=None, scratch=(), aliases={}, dtypes={}):
    specs = [pl.BlockSpec(memory_space=space) for space in in_spaces]
    out_spaces = out_spaces or [pltpu.VMEM] * len(out_shapes)
    operands = [
        operand if space == pltpu.SMEM else pltpu.with_memory_space_constraint(operand, space)
        for operand, space in zip(operands, in_spaces)
    ]
    return kernel_of(body, out_shapes, specs, operands, out_spaces, scratch, aliases, dtypes)


def kernel_of(body, out_shapes, specs, operands, out_spaces, scratch, aliases, dtypes):
    return pl.pallas_call(
        body,
        out_shape=[
            space(shape, dtypes.get(k, jnp.float32))
            if space == pltpu.VMEM
            else jax.ShapeDtypeStruct(shape, jnp.float32)
            for k, (shape, space) in enumerate(zip(out_shapes, out_spaces))
        ],
        in_specs=specs,
        out_specs=[pl.BlockSpec(memory_space=space or pltpu.VMEM) for space in out_spaces],
        scratch_shapes=list(scratch),
        input_output_aliases=aliases,
        compiler_params=pltpu.CompilerParams(vmem_limit_bytes=16 * 2**20),
    )(*operands)


class Plan:
    def __init__(self, tile_rows, tile_cols, patch, modes, slots, lead):
        self.tile_rows, self.tile_cols = tile_rows, tile_cols
        self.patch, self.modes, self.slots = patch, modes, slots
        self.rim = patch // 2
        self.rows = tile_rows + patch
        self.cols = tile_cols + patch
        self.narrow = math.gcd(lead, UNROLL)
        self.broad = math.gcd(modes, BROAD)

    def scratch(self, width, windows=True):
        wide = self.patch
        return (
            [pltpu.VMEM((2, self.rows, self.cols), jnp.float32)]
            + [pltpu.VMEM((self.slots, 2, wide, wide), jnp.float32)] * windows
            + [pltpu.VMEM((width, 2, wide, wide), jnp.bfloat16)] * 2
        )

    def each_unit(self, count, width, body):
        groups = count // width

        def step(index, carry):
            first = lax.rem(index, groups) * width
            body(lax.div(index, groups), [first + j for j in range(width)])
            return carry

        lax.fori_loop(0, self.slots * groups, step, 0)

    def fill_region(self, region, middle, received, weights):
        rim, rows = self.rim, self.tile_rows
        count = len(received)
        low = sum(received[k][...] * weights[k] for k in range(count))
        high = sum(received[k][...] * weights[count + k] for k in range(count))
        region[:, :rim] = low
        region[:, rim : rim + rows] = middle[...]
        region[:, rim + rows :] = high

    def row_split(self, row):
        shift = lax.rem(row, 8)
        return pl.multiple_of(row - shift, 8), shift

    def take_windows(self, windows, region, centres):
        wide = self.patch
        for slot in range(self.slots):
            for part in range(2):
                base, shift = self.row_split(centres[slot, 0])
                strip = region[part, pl.ds(base, wide + 8), :]
                strip = pltpu.roll(strip, wide + 8 - shift, 0)[:wide]
                turned = pltpu.roll(strip, self.cols - centres[slot, 1], 1)
                windows[slot, part] = turned[:, :wide]

    def place(self, canvas, slot, part, piece, centres):
        strip = jnp.concatenate([piece, jnp.zeros((self.patch, self.cols - self.patch), jnp.float32)], 1)
        strip = jnp.concatenate([strip, jnp.zeros((8, self.cols), jnp.float32)], 0)
        base, shift = self.row_split(centres[slot, 0])
        turned = pltpu.roll(pltpu.roll(strip, centres[slot, 1], 1), shift, 0)
        canvas[part, pl.ds(base, self.patch + 8), :] += turned

    def each_modes(self, body):
        def step(index, carry):
            body([index * self.broad + j for j in range(self.broad)])
            return carry

        lax.fori_loop(0, self.modes // self.broad, step, 0)

    def spectra(self, slot, modes, probes, windows, wave, half, tables):
        mid = self.rim
        low, high = slice(0, mid), slice(mid, 2 * mid)
        for top in range(0, mid, 16):
            bands = [slice(top, top + 16), slice(mid + top, mid + top + 16)]
            fields = [[windows[slot, part, band] for part in range(2)] for band in bands]
            for j, mode in enumerate(modes):
                ends = []
                for band, (x_real, x_imag) in zip(bands, fields):
                    p_real, p_imag = probes[mode, 0, band], probes[mode, 1, band]
                    ends.append((p_real * x_real - p_imag * x_imag, p_real * x_imag + p_imag * x_real))
                for part, band in enumerate(bands):
                    wave[j, 0, band] = (ends[0][part] + ends[1][part]).astype(jnp.bfloat16)
                    wave[j, 1, band] = (ends[0][part] - ends[1][part]).astype(jnp.bfloat16)
        for j in range(len(modes)):
            for k, rows in enumerate((low, high)):
                strip = dot(tables[0][k], wave[j, k])
                for part, source in enumerate((low, high)):
                    left, right = strip[source, low], strip[source, high]
                    target = slice(part * mid, (part + 1) * mid)
                    half[j, 0, rows, target] = (left + right).astype(jnp.bfloat16)
                    half[j, 1, rows, target] = (left - right).astype(jnp.bfloat16)
        return [[dot(half[j, k], tables[1][k]) for k in range(2)] for j in range(len(modes))]

    def paired(self, first, second):
        mid = self.rim
        products = [a * b for a, b in zip(first, second)]
        return jnp.concatenate([p[:, :mid] + p[:, mid:] for p in products], 1)

    def load(self, spectra, unit):
        wide = self.patch
        return [spectra[unit, :, :wide], spectra[unit, :, wide:]]

    def store(self, spectra, unit, field):
        wide = self.patch
        spectra[unit, :, :wide], spectra[unit, :, wide:] = field

    def images(self, fields, weight, modes, probes, wave, half, tables):
        mid = self.rim
        low, high = slice(0, mid), slice(mid, 2 * mid)
        doubled = 2.0 * weight
        for j, field in enumerate(fields):
            for k, columns in enumerate((low, high)):
                factor = jnp.concatenate([doubled[:, columns]] * 2, 1)
                half[j, k] = (field[k] * factor).astype(jnp.bfloat16)
        for j in range(len(modes)):
            even, odd = (dot(half[j, k], tables[0][k]) for k in range(2))
            for columns, turned in ((low, even + odd), (high, even - odd)):
                turned = turned.astype(jnp.bfloat16)
                for k, rows in enumerate((low, high)):
                    wave[j, k, low, columns] = turned[rows, low]
                    wave[j, k, high, columns] = turned[rows, high]
        sums = [[0.0, 0.0], [0.0, 0.0]]
        for j, mode in enumerate(modes):
            even, odd = (dot(tables[1][k], wave[j, k]) for k in range(2))
            for side, (rows, back) in enumerate(((low, even + odd), (high, even - odd))):
                p_real, p_imag = probes[mode, 0, rows], probes[mode, 1, rows]
                sums[side][0] = sums[side][0] + (p_real * back[low] + p_imag * back[high])
                sums[side][1] = sums[side][1] + (p_real * back[high] - p_imag * back[low])
        return sums

    def add_images(self, image, sums):
        mid = self.rim
        for side in range(2):
            for part in range(2):
                image[part, side * mid : (side + 1) * mid] += sums[side][part]

    def send(self, canvas, parity, middle_out, sends):
        rim, rows = self.rim, self.tile_rows
        middle_out[...] = canvas[:, rim : rim + rows]
        for k, out in enumerate(sends):
            upper = parity if k == 0 else 1 - parity
            start = pl.multiple_of((1 - upper) * (rim + rows), 8)
            out[...] = canvas[:, pl.ds(start, rim), :]


def start_body(plan, swaps, grid, *refs):
    columns, shards = grid
    info, centres, _, _, windows = refs[:5]
    packed, crossed = refs[5 : 4 + shards], refs[4 + shards : 3 + 2 * shards]
    targets, one, two, probes, spectra, intensity, middle_out, *tail = refs[3 + 2 * shards :]
    sends = tail[:swaps]
    region, wave, half, image, weight = tail[swaps:]
    wide = plan.patch
    lead = plan.modes // shards
    tables = (one, two)
    span = wide // (2 * columns)

    for k in range(1, shards):
        home = source_of(info[PLACE_MA], k, shards) * lead
        for c in range(columns):
            column = source_of(info[PLACE_Y], c, columns) * span
            near = pl.multiple_of(info[SIDE] * (wide // 2) + column, 8)
            far = pl.multiple_of((1 - info[SIDE]) * (wide // 2) + column, 8)
            probes[pl.ds(home, lead), :, pl.ds(near, span), :] = packed[k - 1][c]
            probes[pl.ds(home, lead), :, pl.ds(far, span), :] = crossed[k - 1][c]

    def forward(slot, modes):
        modes = [lax.rem((info[PLACE_MA] + 1) * lead + m, plan.modes) for m in modes]
        fields = plan.spectra(slot, modes, probes, windows, wave, half, tables)
        for mode, field in zip(modes, fields):
            plan.store(spectra, slot * plan.modes + mode, field)

    plan.each_unit(plan.modes - lead, plan.narrow, forward)
    region[...] = jnp.zeros_like(region)
    for slot in range(plan.slots):
        live = jnp.where(slot < info[USED], 1.0, 0.0)

        def brighten(band, carry):
            rows = pl.ds(pl.multiple_of(band * 8, 8), 8)
            power = 0.0
            for mode in range(plan.modes):
                field = spectra[slot * plan.modes + mode, rows]
                pair = [field[:, :wide], field[:, wide:]]
                power = power + plan.paired(pair, pair)
            intensity[slot, rows] = power
            weight[rows] = live * (power - targets[slot, rows])
            return carry

        lax.fori_loop(0, wide // 8, brighten, 0, unroll=4)
        image[...] = jnp.zeros_like(image)

        def backward(modes):
            fields = [plan.load(spectra, slot * plan.modes + mode) for mode in modes]
            sums = plan.images(fields, weight[...], modes, probes, wave, half, tables)
            plan.add_images(image, sums)

        plan.each_modes(backward)
        for part in range(2):
            plan.place(region, slot, part, image[part], centres)
    plan.send(region, info[SIDE], middle_out, sends)


def change_body(plan, swaps, last, *refs):
    refs = list(refs)
    info, centres, weights, middle = refs[:4]
    received = refs[4 : 4 + swaps]
    spectra, probes, one, two = refs[4 + swaps : 8 + swaps]
    outs = refs[8 + swaps :]
    if last:
        sums, region, windows, wave, half, change, power = outs
    else:
        sums, moved, change, power, region, windows, wave, half = outs
    wide, rim = plan.patch, plan.rim
    tables = (one, two)
    plan.fill_region(region, middle, received, weights)
    plan.take_windows(windows, region, centres)
    own = middle[:, :, rim : rim + plan.tile_cols]
    sums[0] = jnp.sum(own * own)
    bend = 0.0
    for slot in range(plan.slots):
        change[slot] = jnp.zeros((wide, wide), jnp.float32)
        if not last:
            power[slot] = jnp.zeros((wide, wide), jnp.float32)

        def forward(modes):
            fields = plan.spectra(slot, modes, probes, windows, wave, half, tables)
            cross = square = 0.0
            for mode, field in zip(modes, fields):
                cross = cross + plan.paired(plan.load(spectra, slot * plan.modes + mode), field)
                if not last:
                    plan.store(moved, slot * plan.modes + mode, field)
                    square = square + plan.paired(field, field)
            change[slot] += 2.0 * cross
            if not last:
                power[slot] += square

        plan.each_modes(forward)
        live = jnp.where(slot < info[USED], 1.0, 0.0)
        bend = bend + live * jnp.sum(change[slot] * change[slot])
    sums[1] = bend


def image_body(plan, swaps, parts, *refs):
    refs = list(refs)
    info, centres = refs[:2]
    totals = refs[2 : 2 + parts]
    spectra, moved, intensity, change, power, probes, targets, one, two = refs[2 + parts : 11 + parts]
    fresh, step_out, middle_out, *tail = refs[11 + parts :]
    sends = tail[:swaps]
    region, windows, wave, half, image = tail[swaps:]
    tables = (one, two)
    step = step_of(totals)
    step_out[0] = step
    region[...] = jnp.zeros_like(region)
    for slot in range(plan.slots):
        live = jnp.where(slot < info[USED], 1.0, 0.0)
        bright = intensity[slot] + step * (change[slot] + step * power[slot])
        windows[slot, 0] = live * (bright - targets[slot])
        image[...] = jnp.zeros_like(image)

        def backward(modes):
            fields = []
            for mode in modes:
                unit = slot * plan.modes + mode
                pairs = zip(plan.load(spectra, unit), plan.load(moved, unit))
                fields.append([base + step * shift for base, shift in pairs])
                plan.store(fresh, unit, fields[-1])
            sums = plan.images(fields, windows[slot, 0], modes, probes, wave, half, tables)
            plan.add_images(image, sums)

        plan.each_modes(backward)
        for part in range(2):
            plan.place(region, slot, part, image[part], centres)
    plan.send(region, info[SIDE], middle_out, sends)


def step_of(totals):
    values = [[part[k] for part in totals] for k in range(2)]
    while len(values[0]) > 1:
        values = [[v[i] + v[i + 1] for i in range(0, len(v), 2)] for v in values]
    norm, bend = values[0][0], values[1][0]
    top = jnp.full((8, 128), norm, jnp.float32)
    return jnp.max(top / (bend + DAMPING * norm))


def pack_body(plan, swaps, columns, *refs):
    info, shard, tile, mine, *rims = refs[: 4 + swaps]
    sems = refs[4 + swaps]
    span = plan.patch // (2 * columns)
    start = pl.multiple_of(info[SIDE] * (plan.patch // 2) + info[PLACE_Y] * span, 8)
    copies = [pltpu.make_async_copy(shard.at[:, :, pl.ds(start, span), :], mine, sems.at[0])]
    for k, rim in enumerate(rims):
        first = jnp.where((info[SIDE_Y] == 0) == (k == 0), plan.tile_cols - plan.rim, 0)
        first = pl.multiple_of(first, 128)
        source = tile.at[:, :, pl.ds(first, plan.rim)]
        copies.append(pltpu.make_async_copy(source, rim, sems.at[1 + k]))
    for copy in copies:
        copy.start()
    for copy in copies:
        copy.wait()


def early_body(plan, swaps, shards, *refs):
    info, centres, weights, middle = refs[:4]
    received = refs[4 : 4 + swaps]
    far_targets, far_one, far_two, far_shard = refs[4 + swaps : 8 + swaps]
    probes, spectra, windows, ordered, one, two = refs[8 + swaps : 14 + swaps]
    region, wave, half, sems = refs[14 + swaps :]
    wide, lead = plan.patch, plan.modes // shards
    home = info[PLACE_MA] * lead
    copies = [
        pltpu.make_async_copy(source, target, sems.at[k])
        for k, (source, target) in enumerate(
            (
                (far_one, one),
                (far_two, two),
                (far_targets, ordered),
                (far_shard, probes.at[pl.ds(home, lead)]),
            )
        )
    ]
    for copy in copies:
        copy.start()
    plan.fill_region(region, middle, received, weights)
    plan.take_windows(windows, region, centres)
    for copy in copies:
        copy.wait()

    place = lax.broadcasted_iota(jnp.int32, (wide, wide), 0)
    source = jnp.where(place < plan.rim, 2 * place, 2 * (place - plan.rim) + 1)
    pick = jnp.where(source == lax.broadcasted_iota(jnp.int32, (wide, wide), 1), 1.0, 0.0)
    pick = pick.astype(jnp.bfloat16)

    def parts_of(block):
        parts = []
        for _ in range(3):
            parts.append(block.astype(jnp.bfloat16))
            block = block - parts[-1].astype(jnp.float32)
        return parts

    for slot in range(plan.slots):
        rows = sum(dot(pick, part) for part in parts_of(ordered[slot]))
        ordered[slot] = sum(
            lax.dot_general(part, pick, (((1,), (1,)), ((), ())), preferred_element_type=jnp.float32)
            for part in parts_of(rows)
        )

    def forward(slot, modes):
        fields = plan.spectra(slot, modes, probes, windows, wave, half, (one, two))
        for mode, field in zip(modes, fields):
            plan.store(spectra, slot * plan.modes + mode, field)

    plan.each_unit(lead, plan.narrow, lambda slot, modes: forward(slot, [home + m for m in modes]))


def widen_body(plan, swaps, *refs):
    weights, tile = refs[:2]
    received = refs[2 : 2 + swaps]
    middle = refs[2 + swaps]
    low, high = sides_of(received, weights)
    middle[:, :, : plan.rim] = low
    middle[:, :, plan.rim : plan.rim + plan.tile_cols] = tile[...]
    middle[:, :, plan.rim + plan.tile_cols :] = high


def join_body(*refs):
    for c, part in enumerate(refs[:-2]):
        refs[-1][c] = part[...]


def sides_of(received, weights):
    count = len(received)
    low = sum(received[k][...] * weights[k] for k in range(count))
    high = sum(received[k][...] * weights[count + k] for k in range(count))
    return low, high


def fold_body(plan, swaps, *refs):
    info, weights, middle = refs[:3]
    received = refs[3 : 3 + swaps]
    merged, *sends = refs[3 + swaps :]
    low, high = sides_of(received, weights)
    merged[...] = middle[...]
    merged[:, : plan.rim] += low
    merged[:, plan.tile_rows - plan.rim :] += high
    for k, out in enumerate(sends):
        left, right = merged[:, :, : plan.patch], merged[:, :, plan.tile_cols :]
        out[...] = jnp.where((info[SIDE_Y] == 0) == (k == 0), right, left)


def halo_body(plan, swaps, *refs):
    weights, inside, merged = refs[:3]
    received = refs[3 : 3 + swaps]
    (middle,) = refs[3 + swaps :]
    low, high = sides_of(received, weights)
    middle[...] = -merged[...]
    middle[:, :, : plan.patch] -= low
    middle[:, :, plan.tile_cols :] -= high
    middle[:, :, : plan.rim] *= inside[0]
    middle[:, :, plan.rim + plan.tile_cols :] *= inside[1]


def finish_body(plan, parts, *refs):
    totals = refs[:parts]
    first_step, tile, first, last, out = refs[parts:]
    span = pl.ds(plan.rim, plan.tile_cols)
    out[...] = tile[...] + first_step[0] * first[:, :, span] + step_of(totals) * last[:, :, span]


def totals_of(sums):
    if lax.axis_size("gx") == 2:
        sums = sums + swap("gx", [sums])[0]
    else:
        sums = lax.psum(sums, "gx")
    count = lax.axis_size("gy")
    if count & (count - 1):
        return [lax.psum(sums, "gy")]
    return [sums] + [lax.ppermute(sums, "gy", pairs) for pairs in exchanges(count)]


def shards(object_field, probe_shard, measured, positions, slot_counts):
    patch = probe_shard.shape[-1]
    tile_rows, tile_cols = object_field.shape[1:]
    columns, groups = lax.axis_size("gy"), lax.axis_size("ma")
    lead = probe_shard.shape[0]
    modes = lead * groups
    slots = measured.shape[2]
    plan = Plan(tile_rows, tile_cols, patch, modes, slots, lead)
    rim, units = plan.rim, slots * modes
    one, two = (jnp.asarray(table) for table in dft_tables(patch))
    targets = measured[0, 0]
    centres = positions[0, 0]
    gx, gy, ma = (lax.axis_index(axis) for axis in ("gx", "gy", "ma"))
    info = jnp.stack([slot_counts[0, 0], ma, gx % 2, gy, gy % 2])
    weights_x, weights_y = side_weights("gx"), side_weights("gy")
    inside = jnp.stack([gy > 0, gy + 1 < columns]).astype(jnp.float32)
    info, centres, weights_x, weights_y, inside = lax.optimization_barrier(
        (info, centres, weights_x, weights_y, inside)
    )
    swaps_x, swaps_y = (len(pair_swaps(lax.axis_size(axis))) for axis in ("gx", "gy"))
    smem, vmem = pltpu.SMEM, pltpu.VMEM
    tall = (2, tile_rows, plan.cols)
    fold = (2, rim, plan.cols)
    image_scratch = pltpu.VMEM((2, patch, patch), jnp.float32)
    span = patch // (2 * columns)

    def rows_around(middle):
        if rim == tile_rows:
            return swap("gx", [middle] * swaps_x)
        even = gx % 2 == 0
        ends = [middle[:, :rim], middle[:, tile_rows - rim :]]
        blocks = [jnp.where(even, ends[1], ends[0]), jnp.where(even, ends[0], ends[1])]
        return swap("gx", blocks[:swaps_x])

    def descent(middle, sends):
        merged, *blocks = call(
            functools.partial(fold_body, plan, swaps_x),
            [tall] + [(2, tile_rows, patch)] * swaps_y,
            [smem] * 2 + [vmem] * (1 + swaps_x),
            [info, weights_x, middle, *swap("gx", sends)],
        )
        (middle,) = call(
            functools.partial(halo_body, plan, swaps_y),
            [tall],
            [smem] * 2 + [vmem] * (1 + swaps_y),
            [weights_y, inside, merged, *swap("gy", blocks)],
        )
        return middle

    hbm, dma = pltpu.HBM, pltpu.SemaphoreType.DMA
    mine, *rims = call(
        functools.partial(pack_body, plan, swaps_y, columns),
        [(lead, 2, span, patch)] + [(2, tile_rows, rim)] * swaps_y,
        [smem] + [hbm] * 2,
        [info, probe_shard, object_field],
        scratch=[dma((1 + swaps_y,))],
    )
    parts = []
    for pairs in exchanges(groups):
        block = lax.ppermute(mine, "ma", pairs)
        across = [lax.ppermute(block, "gy", p) for p in exchanges(columns)]
        parts.append([block, *across])
    (middle,) = call(
        functools.partial(widen_body, plan, swaps_y),
        [tall],
        [smem, vmem] + [vmem] * swaps_y,
        [weights_y, object_field, *swap("gy", rims)],
    )
    probes, spectra, windows, targets, one, two = call(
        functools.partial(early_body, plan, swaps_x, groups),
        [
            (modes, 2, patch, patch),
            (units, patch, 2 * patch),
            (slots, 2, patch, patch),
            targets.shape,
            one.shape,
            two.shape,
        ],
        [smem] * 3 + [vmem] * (1 + swaps_x) + [hbm] * 4,
        [info, centres, weights_x, middle, *rows_around(middle), targets, one, two, probe_shard],
        scratch=plan.scratch(plan.narrow, False) + [dma((4,))],
        dtypes={4: jnp.bfloat16, 5: jnp.bfloat16},
    )
    packed, crossed = [], []
    for blocks in parts:
        packed += call(join_body, [(columns, lead, 2, span, patch)], [vmem] * (columns + 1), [*blocks, windows])
        crossed += swap("gx", packed[-1:])
    probes, spectra, intensity, middle, *sends = call(
        functools.partial(start_body, plan, swaps_x, (columns, groups)),
        [probes.shape, spectra.shape, (slots, patch, patch), tall] + [fold] * swaps_x,
        [smem] * 2 + [vmem] * (6 + 2 * (groups - 1)),
        [info, centres, probes, spectra, windows, *packed, *crossed, targets, one, two],
        scratch=plan.scratch(max(plan.broad, plan.narrow), False)
        + [image_scratch, pltpu.VMEM((patch, patch), jnp.float32)],
        aliases={2: 0, 3: 1},
    )
    first_way = descent(middle, sends)
    sums, moved, change, power = call(
        functools.partial(change_body, plan, swaps_x, False),
        [(2,), (units, patch, 2 * patch), (slots, patch, patch), (slots, patch, patch)],
        [smem] * 3 + [vmem] * (5 + swaps_x),
        [info, centres, weights_x, first_way, *rows_around(first_way), spectra, probes, one, two],
        [smem] + [vmem] * 3,
        scratch=plan.scratch(plan.broad),
    )
    totals = totals_of(sums)
    spectra, first_step, middle, *sends = call(
        functools.partial(image_body, plan, swaps_x, len(totals)),
        [(units, patch, 2 * patch), (1,), tall] + [fold] * swaps_x,
        [smem] * (2 + len(totals)) + [vmem] * 9,
        [info, centres, *totals, spectra, moved, intensity, change, power, probes, targets, one, two],
        [vmem, smem] + [vmem] * (1 + swaps_x),
        scratch=plan.scratch(plan.broad) + [image_scratch],
    )
    last_way = descent(middle, sends)
    (sums,) = call(
        functools.partial(change_body, plan, swaps_x, True),
        [(2,)],
        [smem] * 3 + [vmem] * (5 + swaps_x),
        [info, centres, weights_x, last_way, *rows_around(last_way), spectra, probes, one, two],
        [smem],
        scratch=plan.scratch(plan.broad)
        + [pltpu.VMEM((slots, patch, patch), jnp.float32), pltpu.VMEM((1, 8, 128), jnp.float32)],
    )
    totals = totals_of(sums)
    (current,) = call(
        functools.partial(finish_body, plan, len(totals)),
        [(2, tile_rows, tile_cols)],
        [smem] * (len(totals) + 1) + [vmem] * 3,
        [*totals, first_step, object_field, first_way, last_way],
        [None],
    )
    return current


def solution(mesh):
    return jax.shard_map(
        shards,
        mesh=mesh,
        in_specs=(
            P(None, "gx", "gy"),
            P("ma", None, None, None),
            P("gx", "gy", None, None, None),
            P("gx", "gy", None, None),
            P("gx", "gy"),
        ),
        out_specs=P(None, "gx", "gy"),
        check_vma=False,
    )
```

```python
import functools
import math

import jax
import jax.numpy as jnp
import ml_dtypes
import numpy as np
from jax import lax
from jax.experimental import pallas as pl
from jax.experimental.pallas import tpu as pltpu
from jax.sharding import PartitionSpec as P


DAMPING = 1.0
UNROLL = 2
BROAD = 8
USED, PLACE_MA, SIDE, PLACE_Y, SIDE_Y = range(5)


def dft_tables(width):
    ladder = np.arange(width, dtype=np.int64)
    angles = (ladder[:, None] * ladder[None, : width // 2] % width) * (2.0 * math.pi / width)
    real_part = np.cos(angles) / math.sqrt(width)
    imag_part = -np.sin(angles) / math.sqrt(width)
    blocks = [
        np.block([[real_part[p::2], -imag_part[p::2]], [imag_part[p::2], real_part[p::2]]])
        for p in range(2)
    ]
    one = np.stack(blocks).astype(ml_dtypes.bfloat16)
    return one, np.ascontiguousarray(one.transpose(0, 2, 1))


def pair_swaps(count):
    even = [(i, i ^ 1) for i in range(count) if (i ^ 1) < count]
    if count < 3:
        return [even]
    odd = [(i, i + 1) for i in range(1, count - 1, 2)]
    if count % 2 == 0:
        odd = odd + [(count - 1, 0)]
    return [even, odd + [(target, source) for source, target in odd]]


def side_weights(axis):
    count = lax.axis_size(axis)
    place = lax.axis_index(axis)
    even = place % 2 == 0
    has_low = place > 0
    has_high = place + 1 < count
    flags = [even & has_high, ~even & has_low]
    if count > 2:
        flags = [~even & has_low, even & has_low, even & has_high, ~even & has_high]
    else:
        flags = [~even & has_low, even & has_high]
    return jnp.stack(flags).astype(jnp.float32)


def swap(axis, blocks):
    return [lax.ppermute(block, axis, pairs) for block, pairs in zip(blocks, pair_swaps(lax.axis_size(axis)))]


def exchanges(count):
    if count & (count - 1):
        return [[(i, (i + k) % count) for i in range(count)] for k in range(1, count)]
    return [[(i, i ^ k) for i in range(count)] for k in range(1, count)]


def source_of(place, k, count):
    if count & (count - 1):
        return lax.rem(place - k + count, count)
    return place ^ k


def dot(left, right):
    return jnp.dot(left, right, preferred_element_type=jnp.float32)


def call(body, out_shapes, in_spaces, operands, out_spaces=None, scratch=(), aliases={}, dtypes={}):
    specs = [pl.BlockSpec(memory_space=space) for space in in_spaces]
    out_spaces = out_spaces or [pltpu.VMEM] * len(out_shapes)
    operands = [
        operand if space == pltpu.SMEM else pltpu.with_memory_space_constraint(operand, space)
        for operand, space in zip(operands, in_spaces)
    ]
    return kernel_of(body, out_shapes, specs, operands, out_spaces, scratch, aliases, dtypes)


def kernel_of(body, out_shapes, specs, operands, out_spaces, scratch, aliases, dtypes):
    return pl.pallas_call(
        body,
        out_shape=[
            space(shape, dtypes.get(k, jnp.float32))
            if space == pltpu.VMEM
            else jax.ShapeDtypeStruct(shape, jnp.float32)
            for k, (shape, space) in enumerate(zip(out_shapes, out_spaces))
        ],
        in_specs=specs,
        out_specs=[pl.BlockSpec(memory_space=space or pltpu.VMEM) for space in out_spaces],
        scratch_shapes=list(scratch),
        input_output_aliases=aliases,
        compiler_params=pltpu.CompilerParams(vmem_limit_bytes=16 * 2**20),
    )(*operands)


class Plan:
    def __init__(self, tile_rows, tile_cols, patch, modes, slots, lead):
        self.tile_rows, self.tile_cols = tile_rows, tile_cols
        self.patch, self.modes, self.slots = patch, modes, slots
        self.rim = patch // 2
        self.rows = tile_rows + patch
        self.cols = tile_cols + patch
        self.narrow = math.gcd(lead, UNROLL)
        others = modes - lead
        self.foreign = others if 0 < others <= BROAD else self.narrow
        self.broad = math.gcd(modes, BROAD)

    def scratch(self, width, windows=True):
        wide = self.patch
        return (
            [pltpu.VMEM((2, self.rows, self.cols), jnp.float32)]
            + [pltpu.VMEM((self.slots, 2, wide, wide), jnp.float32)] * windows
            + [pltpu.VMEM((width, 2, wide, wide), jnp.bfloat16)] * 2
        )

    def each_unit(self, count, width, body):
        groups = count // width

        def step(index, carry):
            first = lax.rem(index, groups) * width
            body(lax.div(index, groups), [first + j for j in range(width)])
            return carry

        lax.fori_loop(0, self.slots * groups, step, 0)

    def fill_region(self, region, middle, received, weights):
        rim, rows = self.rim, self.tile_rows
        count = len(received)
        low = sum(received[k][...] * weights[k] for k in range(count))
        high = sum(received[k][...] * weights[count + k] for k in range(count))
        region[:, :rim] = low
        region[:, rim : rim + rows] = middle[...]
        region[:, rim + rows :] = high

    def split(self, place, step):
        shift = lax.rem(place, step)
        return pl.multiple_of(place - shift, step), shift

    def take_windows(self, windows, region, centres):
        wide = self.patch
        for slot in range(self.slots):
            for part in range(2):
                base, shift = self.split(centres[slot, 0], 8)
                first, turn = self.split(centres[slot, 1], 128)
                strip = region[part, pl.ds(base, wide + 8), pl.ds(first, wide + 128)]
                strip = pltpu.roll(strip, wide + 128 - turn, 1)[:, :wide]
                windows[slot, part] = pltpu.roll(strip, wide + 8 - shift, 0)[:wide]

    def place(self, canvas, slot, part, piece, centres):
        wide = self.patch
        base, shift = self.split(centres[slot, 0], 8)
        first, turn = self.split(centres[slot, 1], 128)
        strip = jnp.concatenate([piece, jnp.zeros((8, wide), jnp.float32)], 0)
        strip = pltpu.roll(strip, shift, 0)
        strip = jnp.concatenate([strip, jnp.zeros((wide + 8, 128), jnp.float32)], 1)
        canvas[part, pl.ds(base, wide + 8), pl.ds(first, wide + 128)] += pltpu.roll(strip, turn, 1)

    def each_modes(self, body):
        def step(index, carry):
            body([index * self.broad + j for j in range(self.broad)])
            return carry

        lax.fori_loop(0, self.modes // self.broad, step, 0)

    def spectra(self, slot, modes, probes, windows, wave, half, tables):
        mid = self.rim
        low, high = slice(0, mid), slice(mid, 2 * mid)
        for top in range(0, mid, 16):
            bands = [slice(top, top + 16), slice(mid + top, mid + top + 16)]
            fields = [[windows[slot, part, band] for part in range(2)] for band in bands]
            for j, mode in enumerate(modes):
                ends = []
                for band, (x_real, x_imag) in zip(bands, fields):
                    p_real, p_imag = probes[mode, 0, band], probes[mode, 1, band]
                    ends.append((p_real * x_real - p_imag * x_imag, p_real * x_imag + p_imag * x_real))
                for part, band in enumerate(bands):
                    wave[j, 0, band] = (ends[0][part] + ends[1][part]).astype(jnp.bfloat16)
                    wave[j, 1, band] = (ends[0][part] - ends[1][part]).astype(jnp.bfloat16)
        for j in range(len(modes)):
            for k, rows in enumerate((low, high)):
                strip = dot(tables[0][k], wave[j, k])
                for part, source in enumerate((low, high)):
                    left, right = strip[source, low], strip[source, high]
                    target = slice(part * mid, (part + 1) * mid)
                    half[j, 0, rows, target] = (left + right).astype(jnp.bfloat16)
                    half[j, 1, rows, target] = (left - right).astype(jnp.bfloat16)
        return [[dot(half[j, k], tables[1][k]) for k in range(2)] for j in range(len(modes))]

    def paired(self, first, second):
        mid = self.rim
        products = [a * b for a, b in zip(first, second)]
        return jnp.concatenate([p[:, :mid] + p[:, mid:] for p in products], 1)

    def load(self, spectra, unit):
        wide = self.patch
        return [spectra[unit, :, :wide], spectra[unit, :, wide:]]

    def store(self, spectra, unit, field):
        wide = self.patch
        spectra[unit, :, :wide], spectra[unit, :, wide:] = field

    def images(self, fields, weight, modes, probes, wave, half, tables):
        mid = self.rim
        low, high = slice(0, mid), slice(mid, 2 * mid)
        doubled = 2.0 * weight
        for j, field in enumerate(fields):
            for k, columns in enumerate((low, high)):
                factor = jnp.concatenate([doubled[:, columns]] * 2, 1)
                half[j, k] = (field[k] * factor).astype(jnp.bfloat16)
        for j in range(len(modes)):
            even, odd = (dot(half[j, k], tables[0][k]) for k in range(2))
            for columns, turned in ((low, even + odd), (high, even - odd)):
                turned = turned.astype(jnp.bfloat16)
                for k, rows in enumerate((low, high)):
                    wave[j, k, low, columns] = turned[rows, low]
                    wave[j, k, high, columns] = turned[rows, high]
        sums = [[0.0, 0.0], [0.0, 0.0]]
        for j, mode in enumerate(modes):
            even, odd = (dot(tables[1][k], wave[j, k]) for k in range(2))
            for side, (rows, back) in enumerate(((low, even + odd), (high, even - odd))):
                p_real, p_imag = probes[mode, 0, rows], probes[mode, 1, rows]
                sums[side][0] = sums[side][0] + (p_real * back[low] + p_imag * back[high])
                sums[side][1] = sums[side][1] + (p_real * back[high] - p_imag * back[low])
        return sums

    def add_images(self, image, sums):
        mid = self.rim
        for side in range(2):
            for part in range(2):
                image[part, side * mid : (side + 1) * mid] += sums[side][part]

    def send(self, canvas, parity, middle_out, sends):
        rim, rows = self.rim, self.tile_rows
        middle_out[...] = canvas[:, rim : rim + rows]
        for k, out in enumerate(sends):
            upper = parity if k == 0 else 1 - parity
            start = pl.multiple_of((1 - upper) * (rim + rows), 8)
            out[...] = canvas[:, pl.ds(start, rim), :]


def start_body(plan, swaps, grid, *refs):
    columns, shards = grid
    info, centres, _, _, windows = refs[:5]
    packed, crossed = refs[5 : 4 + shards], refs[4 + shards : 3 + 2 * shards]
    targets, one, two, probes, spectra, intensity, middle_out, *tail = refs[3 + 2 * shards :]
    sends = tail[:swaps]
    region, wave, half, image, weight = tail[swaps:]
    wide = plan.patch
    lead = plan.modes // shards
    tables = (one, two)
    span = wide // (2 * columns)

    for k in range(1, shards):
        home = source_of(info[PLACE_MA], k, shards) * lead
        for c in range(columns):
            column = source_of(info[PLACE_Y], c, columns) * span
            near = pl.multiple_of(info[SIDE] * (wide // 2) + column, 8)
            far = pl.multiple_of((1 - info[SIDE]) * (wide // 2) + column, 8)
            probes[pl.ds(home, lead), :, pl.ds(near, span), :] = packed[k - 1][c]
            probes[pl.ds(home, lead), :, pl.ds(far, span), :] = crossed[k - 1][c]

    def forward(slot, modes):
        modes = [lax.rem((info[PLACE_MA] + 1) * lead + m, plan.modes) for m in modes]
        fields = plan.spectra(slot, modes, probes, windows, wave, half, tables)
        for mode, field in zip(modes, fields):
            plan.store(spectra, slot * plan.modes + mode, field)

    plan.each_unit(plan.modes - lead, plan.foreign, forward)
    region[...] = jnp.zeros_like(region)
    for slot in range(plan.slots):
        live = jnp.where(slot < info[USED], 1.0, 0.0)

        def brighten(band, carry):
            rows = pl.ds(pl.multiple_of(band * 8, 8), 8)
            power = 0.0
            for mode in range(plan.modes):
                field = spectra[slot * plan.modes + mode, rows]
                pair = [field[:, :wide], field[:, wide:]]
                power = power + plan.paired(pair, pair)
            intensity[slot, rows] = power
            weight[rows] = live * (power - targets[slot, rows])
            return carry

        lax.fori_loop(0, wide // 8, brighten, 0, unroll=4)
        image[...] = jnp.zeros_like(image)

        def backward(modes):
            fields = [plan.load(spectra, slot * plan.modes + mode) for mode in modes]
            sums = plan.images(fields, weight[...], modes, probes, wave, half, tables)
            plan.add_images(image, sums)

        plan.each_modes(backward)
        for part in range(2):
            plan.place(region, slot, part, image[part], centres)
    plan.send(region, info[SIDE], middle_out, sends)


def change_body(plan, swaps, last, *refs):
    refs = list(refs)
    info, centres, weights, middle = refs[:4]
    received = refs[4 : 4 + swaps]
    spectra, probes, one, two = refs[4 + swaps : 8 + swaps]
    outs = refs[8 + swaps :]
    if last:
        sums, region, windows, wave, half, change, power = outs
    else:
        sums, moved, change, power, region, windows, wave, half = outs
    wide, rim = plan.patch, plan.rim
    tables = (one, two)
    plan.fill_region(region, middle, received, weights)
    plan.take_windows(windows, region, centres)
    own = middle[:, :, rim : rim + plan.tile_cols]
    sums[0] = jnp.sum(own * own)
    bend = 0.0
    for slot in range(plan.slots):
        change[slot] = jnp.zeros((wide, wide), jnp.float32)
        if not last:
            power[slot] = jnp.zeros((wide, wide), jnp.float32)

        def forward(modes):
            fields = plan.spectra(slot, modes, probes, windows, wave, half, tables)
            cross = square = 0.0
            for mode, field in zip(modes, fields):
                cross = cross + plan.paired(plan.load(spectra, slot * plan.modes + mode), field)
                if not last:
                    plan.store(moved, slot * plan.modes + mode, field)
                    square = square + plan.paired(field, field)
            change[slot] += 2.0 * cross
            if not last:
                power[slot] += square

        plan.each_modes(forward)
        live = jnp.where(slot < info[USED], 1.0, 0.0)
        bend = bend + live * jnp.sum(change[slot] * change[slot])
    sums[1] = bend


def image_body(plan, swaps, parts, *refs):
    refs = list(refs)
    info, centres = refs[:2]
    totals = refs[2 : 2 + parts]
    spectra, moved, intensity, change, power, probes, targets, one, two = refs[2 + parts : 11 + parts]
    fresh, step_out, middle_out, *tail = refs[11 + parts :]
    sends = tail[:swaps]
    region, windows, wave, half, image = tail[swaps:]
    tables = (one, two)
    step = step_of(totals)
    step_out[0] = step
    region[...] = jnp.zeros_like(region)
    for slot in range(plan.slots):
        live = jnp.where(slot < info[USED], 1.0, 0.0)
        bright = intensity[slot] + step * (change[slot] + step * power[slot])
        windows[slot, 0] = live * (bright - targets[slot])
        image[...] = jnp.zeros_like(image)

        def backward(modes):
            fields = []
            for mode in modes:
                unit = slot * plan.modes + mode
                pairs = zip(plan.load(spectra, unit), plan.load(moved, unit))
                fields.append([base + step * shift for base, shift in pairs])
                plan.store(fresh, unit, fields[-1])
            sums = plan.images(fields, windows[slot, 0], modes, probes, wave, half, tables)
            plan.add_images(image, sums)

        plan.each_modes(backward)
        for part in range(2):
            plan.place(region, slot, part, image[part], centres)
    plan.send(region, info[SIDE], middle_out, sends)


def step_of(totals):
    values = [[part[k] for part in totals] for k in range(2)]
    while len(values[0]) > 1:
        values = [[v[i] + v[i + 1] for i in range(0, len(v), 2)] for v in values]
    norm, bend = values[0][0], values[1][0]
    top = jnp.full((8, 128), norm, jnp.float32)
    return jnp.max(top / (bend + DAMPING * norm))


def pack_body(plan, swaps, columns, *refs):
    info, shard, tile, mine, *rims = refs[: 4 + swaps]
    sems = refs[4 + swaps]
    span = plan.patch // (2 * columns)
    start = pl.multiple_of(info[SIDE] * (plan.patch // 2) + info[PLACE_Y] * span, 8)
    copies = [pltpu.make_async_copy(shard.at[:, :, pl.ds(start, span), :], mine, sems.at[0])]
    for k, rim in enumerate(rims):
        first = jnp.where((info[SIDE_Y] == 0) == (k == 0), plan.tile_cols - plan.rim, 0)
        first = pl.multiple_of(first, 128)
        source = tile.at[:, :, pl.ds(first, plan.rim)]
        copies.append(pltpu.make_async_copy(source, rim, sems.at[1 + k]))
    for copy in copies:
        copy.start()
    for copy in copies:
        copy.wait()


def early_body(plan, swaps, shards, *refs):
    info, centres, weights, middle = refs[:4]
    received = refs[4 : 4 + swaps]
    far_targets, far_one, far_two, far_shard = refs[4 + swaps : 8 + swaps]
    probes, spectra, windows, ordered, one, two = refs[8 + swaps : 14 + swaps]
    region, wave, half, sems = refs[14 + swaps :]
    wide, lead = plan.patch, plan.modes // shards
    home = info[PLACE_MA] * lead
    copies = [
        pltpu.make_async_copy(source, target, sems.at[k])
        for k, (source, target) in enumerate(
            (
                (far_one, one),
                (far_two, two),
                (far_targets, ordered),
                (far_shard, probes.at[pl.ds(home, lead)]),
            )
        )
    ]
    for copy in copies:
        copy.start()
    plan.fill_region(region, middle, received, weights)
    plan.take_windows(windows, region, centres)
    for copy in copies:
        copy.wait()

    place = lax.broadcasted_iota(jnp.int32, (wide, wide), 0)
    source = jnp.where(place < plan.rim, 2 * place, 2 * (place - plan.rim) + 1)
    pick = jnp.where(source == lax.broadcasted_iota(jnp.int32, (wide, wide), 1), 1.0, 0.0)
    pick = pick.astype(jnp.bfloat16)

    def parts_of(block):
        parts = []
        for _ in range(3):
            parts.append(block.astype(jnp.bfloat16))
            block = block - parts[-1].astype(jnp.float32)
        return parts

    for slot in range(plan.slots):
        rows = sum(dot(pick, part) for part in parts_of(ordered[slot]))
        ordered[slot] = sum(
            lax.dot_general(part, pick, (((1,), (1,)), ((), ())), preferred_element_type=jnp.float32)
            for part in parts_of(rows)
        )

    def forward(slot, modes):
        fields = plan.spectra(slot, modes, probes, windows, wave, half, (one, two))
        for mode, field in zip(modes, fields):
            plan.store(spectra, slot * plan.modes + mode, field)

    plan.each_unit(lead, plan.narrow, lambda slot, modes: forward(slot, [home + m for m in modes]))


def widen_body(plan, swaps, *refs):
    weights, tile = refs[:2]
    received = refs[2 : 2 + swaps]
    middle = refs[2 + swaps]
    low, high = sides_of(received, weights)
    middle[:, :, : plan.rim] = low
    middle[:, :, plan.rim : plan.rim + plan.tile_cols] = tile[...]
    middle[:, :, plan.rim + plan.tile_cols :] = high


def join_body(*refs):
    for c, part in enumerate(refs[:-2]):
        refs[-1][c] = part[...]


def sides_of(received, weights):
    count = len(received)
    low = sum(received[k][...] * weights[k] for k in range(count))
    high = sum(received[k][...] * weights[count + k] for k in range(count))
    return low, high


def fold_body(plan, swaps, *refs):
    info, weights, middle = refs[:3]
    received = refs[3 : 3 + swaps]
    merged, *sends = refs[3 + swaps :]
    low, high = sides_of(received, weights)
    merged[...] = middle[...]
    merged[:, : plan.rim] += low
    merged[:, plan.tile_rows - plan.rim :] += high
    for k, out in enumerate(sends):
        left, right = merged[:, :, : plan.patch], merged[:, :, plan.tile_cols :]
        out[...] = jnp.where((info[SIDE_Y] == 0) == (k == 0), right, left)


def halo_body(plan, swaps, *refs):
    weights, inside, merged = refs[:3]
    received = refs[3 : 3 + swaps]
    (middle,) = refs[3 + swaps :]
    low, high = sides_of(received, weights)
    middle[...] = -merged[...]
    middle[:, :, : plan.patch] -= low
    middle[:, :, plan.tile_cols :] -= high
    middle[:, :, : plan.rim] *= inside[0]
    middle[:, :, plan.rim + plan.tile_cols :] *= inside[1]


def finish_body(plan, parts, *refs):
    totals = refs[:parts]
    first_step, tile, first, last, out = refs[parts:]
    span = pl.ds(plan.rim, plan.tile_cols)
    out[...] = tile[...] + first_step[0] * first[:, :, span] + step_of(totals) * last[:, :, span]


def totals_of(sums):
    if lax.axis_size("gx") == 2:
        sums = sums + swap("gx", [sums])[0]
    else:
        sums = lax.psum(sums, "gx")
    count = lax.axis_size("gy")
    if count & (count - 1):
        return [lax.psum(sums, "gy")]
    return [sums] + [lax.ppermute(sums, "gy", pairs) for pairs in exchanges(count)]


def shards(object_field, probe_shard, measured, positions, slot_counts):
    patch = probe_shard.shape[-1]
    tile_rows, tile_cols = object_field.shape[1:]
    columns, groups = lax.axis_size("gy"), lax.axis_size("ma")
    lead = probe_shard.shape[0]
    modes = lead * groups
    slots = measured.shape[2]
    plan = Plan(tile_rows, tile_cols, patch, modes, slots, lead)
    rim, units = plan.rim, slots * modes
    one, two = (jnp.asarray(table) for table in dft_tables(patch))
    targets = measured[0, 0]
    centres = positions[0, 0]
    gx, gy, ma = (lax.axis_index(axis) for axis in ("gx", "gy", "ma"))
    info = jnp.stack([slot_counts[0, 0], ma, gx % 2, gy, gy % 2])
    weights_x, weights_y = side_weights("gx"), side_weights("gy")
    inside = jnp.stack([gy > 0, gy + 1 < columns]).astype(jnp.float32)
    info, centres, weights_x, weights_y, inside = lax.optimization_barrier(
        (info, centres, weights_x, weights_y, inside)
    )
    swaps_x, swaps_y = (len(pair_swaps(lax.axis_size(axis))) for axis in ("gx", "gy"))
    smem, vmem = pltpu.SMEM, pltpu.VMEM
    tall = (2, tile_rows, plan.cols)
    fold = (2, rim, plan.cols)
    image_scratch = pltpu.VMEM((2, patch, patch), jnp.float32)
    span = patch // (2 * columns)

    def rows_around(middle):
        if rim == tile_rows:
            return swap("gx", [middle] * swaps_x)
        even = gx % 2 == 0
        ends = [middle[:, :rim], middle[:, tile_rows - rim :]]
        blocks = [jnp.where(even, ends[1], ends[0]), jnp.where(even, ends[0], ends[1])]
        return swap("gx", blocks[:swaps_x])

    def descent(middle, sends):
        merged, *blocks = call(
            functools.partial(fold_body, plan, swaps_x),
            [tall] + [(2, tile_rows, patch)] * swaps_y,
            [smem] * 2 + [vmem] * (1 + swaps_x),
            [info, weights_x, middle, *swap("gx", sends)],
        )
        (middle,) = call(
            functools.partial(halo_body, plan, swaps_y),
            [tall],
            [smem] * 2 + [vmem] * (1 + swaps_y),
            [weights_y, inside, merged, *swap("gy", blocks)],
        )
        return middle

    hbm, dma = pltpu.HBM, pltpu.SemaphoreType.DMA
    mine, *rims = call(
        functools.partial(pack_body, plan, swaps_y, columns),
        [(lead, 2, span, patch)] + [(2, tile_rows, rim)] * swaps_y,
        [smem] + [hbm] * 2,
        [info, probe_shard, object_field],
        scratch=[dma((1 + swaps_y,))],
    )
    parts = []
    for pairs in exchanges(groups):
        block = lax.ppermute(mine, "ma", pairs)
        across = [lax.ppermute(block, "gy", p) for p in exchanges(columns)]
        parts.append([block, *across])
    (middle,) = call(
        functools.partial(widen_body, plan, swaps_y),
        [tall],
        [smem, vmem] + [vmem] * swaps_y,
        [weights_y, object_field, *swap("gy", rims)],
    )
    probes, spectra, windows, targets, one, two = call(
        functools.partial(early_body, plan, swaps_x, groups),
        [
            (modes, 2, patch, patch),
            (units, patch, 2 * patch),
            (slots, 2, patch, patch),
            targets.shape,
            one.shape,
            two.shape,
        ],
        [smem] * 3 + [vmem] * (1 + swaps_x) + [hbm] * 4,
        [info, centres, weights_x, middle, *rows_around(middle), targets, one, two, probe_shard],
        scratch=plan.scratch(plan.narrow, False) + [dma((4,))],
        dtypes={4: jnp.bfloat16, 5: jnp.bfloat16},
    )
    packed, crossed = [], []
    for blocks in parts:
        packed += call(join_body, [(columns, lead, 2, span, patch)], [vmem] * (columns + 1), [*blocks, windows])
        crossed += swap("gx", packed[-1:])
    probes, spectra, intensity, middle, *sends = call(
        functools.partial(start_body, plan, swaps_x, (columns, groups)),
        [probes.shape, spectra.shape, (slots, patch, patch), tall] + [fold] * swaps_x,
        [smem] * 2 + [vmem] * (6 + 2 * (groups - 1)),
        [info, centres, probes, spectra, windows, *packed, *crossed, targets, one, two],
        scratch=plan.scratch(max(plan.broad, plan.foreign), False)
        + [image_scratch, pltpu.VMEM((patch, patch), jnp.float32)],
        aliases={2: 0, 3: 1},
    )
    first_way = descent(middle, sends)
    sums, moved, change, power = call(
        functools.partial(change_body, plan, swaps_x, False),
        [(2,), (units, patch, 2 * patch), (slots, patch, patch), (slots, patch, patch)],
        [smem] * 3 + [vmem] * (5 + swaps_x),
        [info, centres, weights_x, first_way, *rows_around(first_way), spectra, probes, one, two],
        [smem] + [vmem] * 3,
        scratch=plan.scratch(plan.broad),
    )
    totals = totals_of(sums)
    spectra, first_step, middle, *sends = call(
        functools.partial(image_body, plan, swaps_x, len(totals)),
        [(units, patch, 2 * patch), (1,), tall] + [fold] * swaps_x,
        [smem] * (2 + len(totals)) + [vmem] * 9,
        [info, centres, *totals, spectra, moved, intensity, change, power, probes, targets, one, two],
        [vmem, smem] + [vmem] * (1 + swaps_x),
        scratch=plan.scratch(plan.broad) + [image_scratch],
    )
    last_way = descent(middle, sends)
    (sums,) = call(
        functools.partial(change_body, plan, swaps_x, True),
        [(2,)],
        [smem] * 3 + [vmem] * (5 + swaps_x),
        [info, centres, weights_x, last_way, *rows_around(last_way), spectra, probes, one, two],
        [smem],
        scratch=plan.scratch(plan.broad)
        + [pltpu.VMEM((slots, patch, patch), jnp.float32), pltpu.VMEM((1, 8, 128), jnp.float32)],
    )
    totals = totals_of(sums)
    (current,) = call(
        functools.partial(finish_body, plan, len(totals)),
        [(2, tile_rows, tile_cols)],
        [smem] * (len(totals) + 1) + [vmem] * 3,
        [*totals, first_step, object_field, first_way, last_way],
        [None],
    )
    return current


def solution(mesh):
    return jax.shard_map(
        shards,
        mesh=mesh,
        in_specs=(
            P(None, "gx", "gy"),
            P("ma", None, None, None),
            P("gx", "gy", None, None, None),
            P("gx", "gy", None, None),
            P("gx", "gy"),
        ),
        out_specs=P(None, "gx", "gy"),
        check_vma=False,
    )
```

```python
import functools
import math

import jax
import jax.numpy as jnp
import ml_dtypes
import numpy as np
from jax import lax
from jax.experimental import pallas as pl
from jax.experimental.pallas import tpu as pltpu
from jax.sharding import PartitionSpec as P


DAMPING = 1.0
UNROLL = 2
UNDER = 1
BROAD = 8
USED, PLACE_MA, SIDE, PLACE_Y, SIDE_Y = range(5)


def dft_tables(width):
    ladder = np.arange(width, dtype=np.int64)
    angles = (ladder[:, None] * ladder[None, : width // 2] % width) * (2.0 * math.pi / width)
    real_part = np.cos(angles) / math.sqrt(width)
    imag_part = -np.sin(angles) / math.sqrt(width)
    blocks = [
        np.block([[real_part[p::2], -imag_part[p::2]], [imag_part[p::2], real_part[p::2]]])
        for p in range(2)
    ]
    one = np.stack(blocks).astype(ml_dtypes.bfloat16)
    return one, np.ascontiguousarray(one.transpose(0, 2, 1))


def pair_swaps(count):
    even = [(i, i ^ 1) for i in range(count) if (i ^ 1) < count]
    if count < 3:
        return [even]
    odd = [(i, i + 1) for i in range(1, count - 1, 2)]
    if count % 2 == 0:
        odd = odd + [(count - 1, 0)]
    return [even, odd + [(target, source) for source, target in odd]]


def side_weights(axis):
    count = lax.axis_size(axis)
    place = lax.axis_index(axis)
    even = place % 2 == 0
    has_low = place > 0
    has_high = place + 1 < count
    flags = [even & has_high, ~even & has_low]
    if count > 2:
        flags = [~even & has_low, even & has_low, even & has_high, ~even & has_high]
    else:
        flags = [~even & has_low, even & has_high]
    return jnp.stack(flags).astype(jnp.float32)


def swap(axis, blocks):
    return [lax.ppermute(block, axis, pairs) for block, pairs in zip(blocks, pair_swaps(lax.axis_size(axis)))]


def exchanges(count):
    if count & (count - 1):
        return [[(i, (i + k) % count) for i in range(count)] for k in range(1, count)]
    return [[(i, i ^ k) for i in range(count)] for k in range(1, count)]


def source_of(place, k, count):
    if count & (count - 1):
        return lax.rem(place - k + count, count)
    return place ^ k


def dot(left, right):
    return jnp.dot(left, right, preferred_element_type=jnp.float32)


def call(body, out_shapes, in_spaces, operands, out_spaces=None, scratch=(), aliases={}, dtypes={}):
    specs = [pl.BlockSpec(memory_space=space) for space in in_spaces]
    out_spaces = out_spaces or [pltpu.VMEM] * len(out_shapes)
    operands = [
        operand if space == pltpu.SMEM else pltpu.with_memory_space_constraint(operand, space)
        for operand, space in zip(operands, in_spaces)
    ]
    return kernel_of(body, out_shapes, specs, operands, out_spaces, scratch, aliases, dtypes)


def kernel_of(body, out_shapes, specs, operands, out_spaces, scratch, aliases, dtypes):
    return pl.pallas_call(
        body,
        out_shape=[
            space(shape, dtypes.get(k, jnp.float32))
            if space == pltpu.VMEM
            else jax.ShapeDtypeStruct(shape, jnp.float32)
            for k, (shape, space) in enumerate(zip(out_shapes, out_spaces))
        ],
        in_specs=specs,
        out_specs=[pl.BlockSpec(memory_space=space or pltpu.VMEM) for space in out_spaces],
        scratch_shapes=list(scratch),
        input_output_aliases=aliases,
        compiler_params=pltpu.CompilerParams(vmem_limit_bytes=16 * 2**20),
    )(*operands)


class Plan:
    def __init__(self, tile_rows, tile_cols, patch, modes, slots, lead):
        self.tile_rows, self.tile_cols = tile_rows, tile_cols
        self.patch, self.modes, self.slots = patch, modes, slots
        self.rim = patch // 2
        self.rows = tile_rows + patch
        self.cols = tile_cols + patch
        self.narrow = math.gcd(lead, UNROLL)
        others = modes - lead
        self.foreign = others if 0 < others <= BROAD else self.narrow
        self.broad = math.gcd(modes, BROAD)

    def scratch(self, width, windows=True):
        wide = self.patch
        return (
            [pltpu.VMEM((2, self.rows, self.cols), jnp.float32)]
            + [pltpu.VMEM((self.slots, 2, wide, wide), jnp.float32)] * windows
            + [pltpu.VMEM((width, 2, wide, wide), jnp.bfloat16)] * 2
        )

    def each_unit(self, count, width, body):
        groups = count // width

        def step(index, carry):
            first = lax.rem(index, groups) * width
            body(lax.div(index, groups), [first + j for j in range(width)])
            return carry

        lax.fori_loop(0, self.slots * groups, step, 0)

    def fill_region(self, region, middle, received, weights):
        rim, rows = self.rim, self.tile_rows
        count = len(received)
        low = sum(received[k][...] * weights[k] for k in range(count))
        high = sum(received[k][...] * weights[count + k] for k in range(count))
        region[:, :rim] = low
        region[:, rim : rim + rows] = middle[...]
        region[:, rim + rows :] = high

    def split(self, place, step):
        shift = lax.rem(place, step)
        return pl.multiple_of(place - shift, step), shift

    def take_windows(self, windows, region, centres):
        wide = self.patch
        for slot in range(self.slots):
            for part in range(2):
                base, shift = self.split(centres[slot, 0], 8)
                first, turn = self.split(centres[slot, 1], 128)
                strip = region[part, pl.ds(base, wide + 8), pl.ds(first, wide + 128)]
                strip = pltpu.roll(strip, wide + 128 - turn, 1)[:, :wide]
                windows[slot, part] = pltpu.roll(strip, wide + 8 - shift, 0)[:wide]

    def place(self, canvas, slot, part, piece, centres):
        wide = self.patch
        base, shift = self.split(centres[slot, 0], 8)
        first, turn = self.split(centres[slot, 1], 128)
        strip = jnp.concatenate([piece, jnp.zeros((8, wide), jnp.float32)], 0)
        strip = pltpu.roll(strip, shift, 0)
        strip = jnp.concatenate([strip, jnp.zeros((wide + 8, 128), jnp.float32)], 1)
        canvas[part, pl.ds(base, wide + 8), pl.ds(first, wide + 128)] += pltpu.roll(strip, turn, 1)

    def each_modes(self, body):
        def step(index, carry):
            body([index * self.broad + j for j in range(self.broad)])
            return carry

        lax.fori_loop(0, self.modes // self.broad, step, 0)

    def spectra(self, slot, modes, probes, windows, wave, half, tables):
        mid = self.rim
        low, high = slice(0, mid), slice(mid, 2 * mid)
        for top in range(0, mid, 16):
            bands = [slice(top, top + 16), slice(mid + top, mid + top + 16)]
            fields = [[windows[slot, part, band] for part in range(2)] for band in bands]
            for j, mode in enumerate(modes):
                ends = []
                for band, (x_real, x_imag) in zip(bands, fields):
                    p_real, p_imag = probes[mode, 0, band], probes[mode, 1, band]
                    ends.append((p_real * x_real - p_imag * x_imag, p_real * x_imag + p_imag * x_real))
                for part, band in enumerate(bands):
                    wave[j, 0, band] = (ends[0][part] + ends[1][part]).astype(jnp.bfloat16)
                    wave[j, 1, band] = (ends[0][part] - ends[1][part]).astype(jnp.bfloat16)
        for j in range(len(modes)):
            for k, rows in enumerate((low, high)):
                strip = dot(tables[0][k], wave[j, k])
                for part, source in enumerate((low, high)):
                    left, right = strip[source, low], strip[source, high]
                    target = slice(part * mid, (part + 1) * mid)
                    half[j, 0, rows, target] = (left + right).astype(jnp.bfloat16)
                    half[j, 1, rows, target] = (left - right).astype(jnp.bfloat16)
        return [[dot(half[j, k], tables[1][k]) for k in range(2)] for j in range(len(modes))]

    def paired(self, first, second):
        mid = self.rim
        products = [a * b for a, b in zip(first, second)]
        return jnp.concatenate([p[:, :mid] + p[:, mid:] for p in products], 1)

    def load(self, spectra, unit):
        wide = self.patch
        return [spectra[unit, :, :wide], spectra[unit, :, wide:]]

    def store(self, spectra, unit, field):
        wide = self.patch
        spectra[unit, :, :wide], spectra[unit, :, wide:] = field

    def images(self, fields, weight, modes, probes, wave, half, tables):
        mid = self.rim
        low, high = slice(0, mid), slice(mid, 2 * mid)
        doubled = 2.0 * weight
        for j, field in enumerate(fields):
            for k, columns in enumerate((low, high)):
                factor = jnp.concatenate([doubled[:, columns]] * 2, 1)
                half[j, k] = (field[k] * factor).astype(jnp.bfloat16)
        for j in range(len(modes)):
            even, odd = (dot(half[j, k], tables[0][k]) for k in range(2))
            for columns, turned in ((low, even + odd), (high, even - odd)):
                turned = turned.astype(jnp.bfloat16)
                for k, rows in enumerate((low, high)):
                    wave[j, k, low, columns] = turned[rows, low]
                    wave[j, k, high, columns] = turned[rows, high]
        sums = [[0.0, 0.0], [0.0, 0.0]]
        for j, mode in enumerate(modes):
            even, odd = (dot(tables[1][k], wave[j, k]) for k in range(2))
            for side, (rows, back) in enumerate(((low, even + odd), (high, even - odd))):
                p_real, p_imag = probes[mode, 0, rows], probes[mode, 1, rows]
                sums[side][0] = sums[side][0] + (p_real * back[low] + p_imag * back[high])
                sums[side][1] = sums[side][1] + (p_real * back[high] - p_imag * back[low])
        return sums

    def add_images(self, image, sums):
        mid = self.rim
        for side in range(2):
            for part in range(2):
                image[part, side * mid : (side + 1) * mid] += sums[side][part]

    def send(self, canvas, parity, middle_out, sends):
        rim, rows = self.rim, self.tile_rows
        middle_out[...] = canvas[:, rim : rim + rows]
        for k, out in enumerate(sends):
            upper = parity if k == 0 else 1 - parity
            start = pl.multiple_of((1 - upper) * (rim + rows), 8)
            out[...] = canvas[:, pl.ds(start, rim), :]


def start_body(plan, swaps, grid, *refs):
    columns, shards = grid
    info, centres, _, _, windows = refs[:5]
    packed, crossed = refs[5 : 4 + shards], refs[4 + shards : 3 + 2 * shards]
    targets, one, two, probes, spectra, intensity, middle_out, *tail = refs[3 + 2 * shards :]
    sends = tail[:swaps]
    region, wave, half, image, weight = tail[swaps:]
    wide = plan.patch
    lead = plan.modes // shards
    tables = (one, two)
    span = wide // (2 * columns)

    for k in range(1, shards):
        home = source_of(info[PLACE_MA], k, shards) * lead
        for c in range(columns):
            column = source_of(info[PLACE_Y], c, columns) * span
            near = pl.multiple_of(info[SIDE] * (wide // 2) + column, 8)
            far = pl.multiple_of((1 - info[SIDE]) * (wide // 2) + column, 8)
            probes[pl.ds(home, lead), :, pl.ds(near, span), :] = packed[k - 1][c]
            probes[pl.ds(home, lead), :, pl.ds(far, span), :] = crossed[k - 1][c]

    def forward(slot, modes):
        modes = [lax.rem((info[PLACE_MA] + 1) * lead + m, plan.modes) for m in modes]
        fields = plan.spectra(slot, modes, probes, windows, wave, half, tables)
        for mode, field in zip(modes, fields):
            plan.store(spectra, slot * plan.modes + mode, field)

    plan.each_unit(plan.modes - lead, plan.foreign, forward)
    region[...] = jnp.zeros_like(region)
    for slot in range(plan.slots):
        live = jnp.where(slot < info[USED], 1.0, 0.0)

        def brighten(band, carry):
            rows = pl.ds(pl.multiple_of(band * 8, 8), 8)
            power = 0.0
            for mode in range(plan.modes):
                field = spectra[slot * plan.modes + mode, rows]
                pair = [field[:, :wide], field[:, wide:]]
                power = power + plan.paired(pair, pair)
            intensity[slot, rows] = power
            weight[rows] = live * (power - targets[slot, rows])
            return carry

        lax.fori_loop(0, wide // 8, brighten, 0, unroll=4)
        image[...] = jnp.zeros_like(image)

        def backward(modes):
            fields = [plan.load(spectra, slot * plan.modes + mode) for mode in modes]
            sums = plan.images(fields, weight[...], modes, probes, wave, half, tables)
            plan.add_images(image, sums)

        plan.each_modes(backward)
        for part in range(2):
            plan.place(region, slot, part, image[part], centres)
    plan.send(region, info[SIDE], middle_out, sends)


def change_body(plan, swaps, last, *refs):
    refs = list(refs)
    info, centres, weights, middle = refs[:4]
    received = refs[4 : 4 + swaps]
    spectra, probes, one, two = refs[4 + swaps : 8 + swaps]
    outs = refs[8 + swaps :]
    if last:
        sums, region, windows, wave, half, change, power = outs
    else:
        sums, moved, change, power, region, windows, wave, half = outs
    wide, rim = plan.patch, plan.rim
    tables = (one, two)
    plan.fill_region(region, middle, received, weights)
    plan.take_windows(windows, region, centres)
    own = middle[:, :, rim : rim + plan.tile_cols]
    sums[0] = jnp.sum(own * own)
    bend = 0.0
    for slot in range(plan.slots):
        change[slot] = jnp.zeros((wide, wide), jnp.float32)
        if not last:
            power[slot] = jnp.zeros((wide, wide), jnp.float32)

        def forward(modes):
            fields = plan.spectra(slot, modes, probes, windows, wave, half, tables)
            cross = square = 0.0
            for mode, field in zip(modes, fields):
                cross = cross + plan.paired(plan.load(spectra, slot * plan.modes + mode), field)
                if not last:
                    plan.store(moved, slot * plan.modes + mode, field)
                    square = square + plan.paired(field, field)
            change[slot] += 2.0 * cross
            if not last:
                power[slot] += square

        plan.each_modes(forward)
        live = jnp.where(slot < info[USED], 1.0, 0.0)
        bend = bend + live * jnp.sum(change[slot] * change[slot])
    sums[1] = bend


def image_body(plan, swaps, parts, *refs):
    refs = list(refs)
    info, centres = refs[:2]
    totals = refs[2 : 2 + parts]
    spectra, moved, intensity, change, power, probes, targets, one, two = refs[2 + parts : 11 + parts]
    fresh, step_out, middle_out, *tail = refs[11 + parts :]
    sends = tail[:swaps]
    region, windows, wave, half, image = tail[swaps:]
    tables = (one, two)
    step = step_of(totals)
    step_out[0] = step
    region[...] = jnp.zeros_like(region)
    for slot in range(plan.slots):
        live = jnp.where(slot < info[USED], 1.0, 0.0)
        bright = intensity[slot] + step * (change[slot] + step * power[slot])
        windows[slot, 0] = live * (bright - targets[slot])
        image[...] = jnp.zeros_like(image)

        def backward(modes):
            fields = []
            for mode in modes:
                unit = slot * plan.modes + mode
                pairs = zip(plan.load(spectra, unit), plan.load(moved, unit))
                fields.append([base + step * shift for base, shift in pairs])
                plan.store(fresh, unit, fields[-1])
            sums = plan.images(fields, windows[slot, 0], modes, probes, wave, half, tables)
            plan.add_images(image, sums)

        plan.each_modes(backward)
        for part in range(2):
            plan.place(region, slot, part, image[part], centres)
    plan.send(region, info[SIDE], middle_out, sends)


def step_of(totals):
    values = [[part[k] for part in totals] for k in range(2)]
    while len(values[0]) > 1:
        values = [[v[i] + v[i + 1] for i in range(0, len(v), 2)] for v in values]
    norm, bend = values[0][0], values[1][0]
    top = jnp.full((8, 128), norm, jnp.float32)
    return jnp.max(top / (bend + DAMPING * norm))


def pack_body(plan, swaps, columns, *refs):
    info, shard, tile, mine, near_tile, *rims = refs[: 5 + swaps]
    sems = refs[5 + swaps]
    span = plan.patch // (2 * columns)
    start = pl.multiple_of(info[SIDE] * (plan.patch // 2) + info[PLACE_Y] * span, 8)
    copies = [pltpu.make_async_copy(shard.at[:, :, pl.ds(start, span), :], mine, sems.at[0])]
    for k, rim in enumerate(rims):
        first = jnp.where((info[SIDE_Y] == 0) == (k == 0), plan.tile_cols - plan.rim, 0)
        first = pl.multiple_of(first, 128)
        source = tile.at[:, :, pl.ds(first, plan.rim)]
        copies.append(pltpu.make_async_copy(source, rim, sems.at[1 + k]))
    copies.append(pltpu.make_async_copy(tile, near_tile, sems.at[1 + swaps]))
    for copy in copies:
        copy.start()
    for copy in copies:
        copy.wait()


def early_body(plan, swaps, shards, *refs):
    info, centres, weights, middle = refs[:4]
    received = refs[4 : 4 + swaps]
    far_targets, far_one, far_two, far_shard = refs[4 + swaps : 8 + swaps]
    probes, spectra, windows, ordered, one, two = refs[8 + swaps : 14 + swaps]
    region, wave, half, sems = refs[14 + swaps :]
    wide, lead = plan.patch, plan.modes // shards
    home = info[PLACE_MA] * lead
    copies = [
        pltpu.make_async_copy(source, target, sems.at[k])
        for k, (source, target) in enumerate(
            (
                (far_one, one),
                (far_two, two),
                (far_targets, ordered),
                (far_shard, probes.at[pl.ds(home, lead)]),
            )
        )
    ]
    for copy in copies:
        copy.start()
    plan.fill_region(region, middle, received, weights)
    plan.take_windows(windows, region, centres)
    for copy in copies:
        copy.wait()

    place = lax.broadcasted_iota(jnp.int32, (wide, wide), 0)
    source = jnp.where(place < plan.rim, 2 * place, 2 * (place - plan.rim) + 1)
    pick = jnp.where(source == lax.broadcasted_iota(jnp.int32, (wide, wide), 1), 1.0, 0.0)
    pick = pick.astype(jnp.bfloat16)

    def parts_of(block):
        parts = []
        for _ in range(3):
            parts.append(block.astype(jnp.bfloat16))
            block = block - parts[-1].astype(jnp.float32)
        return parts

    for slot in range(plan.slots):
        rows = sum(dot(pick, part) for part in parts_of(ordered[slot]))
        ordered[slot] = sum(
            lax.dot_general(part, pick, (((1,), (1,)), ((), ())), preferred_element_type=jnp.float32)
            for part in parts_of(rows)
        )

    def forward(slot, modes):
        fields = plan.spectra(slot, modes, probes, windows, wave, half, (one, two))
        for mode, field in zip(modes, fields):
            plan.store(spectra, slot * plan.modes + mode, field)

    plan.each_unit(lead, plan.narrow, lambda slot, modes: forward(slot, [home + m for m in modes]))


def widen_body(plan, swaps, *refs):
    weights, tile = refs[:2]
    received = refs[2 : 2 + swaps]
    middle = refs[2 + swaps]
    low, high = sides_of(received, weights)
    middle[:, :, : plan.rim] = low
    middle[:, :, plan.rim : plan.rim + plan.tile_cols] = tile[...]
    middle[:, :, plan.rim + plan.tile_cols :] = high


def join_body(*refs):
    for c, part in enumerate(refs[:-2]):
        refs[-1][c] = part[...]


def sides_of(received, weights):
    count = len(received)
    low = sum(received[k][...] * weights[k] for k in range(count))
    high = sum(received[k][...] * weights[count + k] for k in range(count))
    return low, high


def fold_body(plan, swaps, *refs):
    info, weights, middle = refs[:3]
    received = refs[3 : 3 + swaps]
    merged, *sends = refs[3 + swaps :]
    low, high = sides_of(received, weights)
    merged[...] = middle[...]
    merged[:, : plan.rim] += low
    merged[:, plan.tile_rows - plan.rim :] += high
    for k, out in enumerate(sends):
        left, right = merged[:, :, : plan.patch], merged[:, :, plan.tile_cols :]
        out[...] = jnp.where((info[SIDE_Y] == 0) == (k == 0), right, left)


def halo_body(plan, swaps, *refs):
    weights, inside, merged = refs[:3]
    received = refs[3 : 3 + swaps]
    (middle,) = refs[3 + swaps :]
    low, high = sides_of(received, weights)
    middle[...] = -merged[...]
    middle[:, :, : plan.patch] -= low
    middle[:, :, plan.tile_cols :] -= high
    middle[:, :, : plan.rim] *= inside[0]
    middle[:, :, plan.rim + plan.tile_cols :] *= inside[1]


def finish_body(plan, parts, *refs):
    totals = refs[:parts]
    first_step, tile, first, last, out = refs[parts:]
    span = pl.ds(plan.rim, plan.tile_cols)
    out[...] = tile[...] + first_step[0] * first[:, :, span] + step_of(totals) * last[:, :, span]


def totals_of(sums):
    if lax.axis_size("gx") == 2:
        sums = sums + swap("gx", [sums])[0]
    else:
        sums = lax.psum(sums, "gx")
    count = lax.axis_size("gy")
    if count & (count - 1):
        return [lax.psum(sums, "gy")]
    return [sums] + [lax.ppermute(sums, "gy", pairs) for pairs in exchanges(count)]


def shards(object_field, probe_shard, measured, positions, slot_counts):
    patch = probe_shard.shape[-1]
    tile_rows, tile_cols = object_field.shape[1:]
    columns, groups = lax.axis_size("gy"), lax.axis_size("ma")
    lead = probe_shard.shape[0]
    modes = lead * groups
    slots = measured.shape[2]
    plan = Plan(tile_rows, tile_cols, patch, modes, slots, lead)
    rim, units = plan.rim, slots * modes
    one, two = (jnp.asarray(table) for table in dft_tables(patch))
    targets = measured[0, 0]
    centres = positions[0, 0]
    gx, gy, ma = (lax.axis_index(axis) for axis in ("gx", "gy", "ma"))
    info = jnp.stack([slot_counts[0, 0], ma, gx % 2, gy, gy % 2])
    weights_x, weights_y = side_weights("gx"), side_weights("gy")
    inside = jnp.stack([gy > 0, gy + 1 < columns]).astype(jnp.float32)
    info, centres, weights_x, weights_y, inside = lax.optimization_barrier(
        (info, centres, weights_x, weights_y, inside)
    )
    swaps_x, swaps_y = (len(pair_swaps(lax.axis_size(axis))) for axis in ("gx", "gy"))
    smem, vmem = pltpu.SMEM, pltpu.VMEM
    tall = (2, tile_rows, plan.cols)
    fold = (2, rim, plan.cols)
    image_scratch = pltpu.VMEM((2, patch, patch), jnp.float32)
    span = patch // (2 * columns)

    def rows_around(middle):
        if rim == tile_rows:
            return swap("gx", [middle] * swaps_x)
        even = gx % 2 == 0
        ends = [middle[:, :rim], middle[:, tile_rows - rim :]]
        blocks = [jnp.where(even, ends[1], ends[0]), jnp.where(even, ends[0], ends[1])]
        return swap("gx", blocks[:swaps_x])

    def descent(middle, sends):
        merged, *blocks = call(
            functools.partial(fold_body, plan, swaps_x),
            [tall] + [(2, tile_rows, patch)] * swaps_y,
            [smem] * 2 + [vmem] * (1 + swaps_x),
            [info, weights_x, middle, *swap("gx", sends)],
        )
        (middle,) = call(
            functools.partial(halo_body, plan, swaps_y),
            [tall],
            [smem] * 2 + [vmem] * (1 + swaps_y),
            [weights_y, inside, merged, *swap("gy", blocks)],
        )
        return middle

    hbm, dma = pltpu.HBM, pltpu.SemaphoreType.DMA
    mine, near_tile, *rims = call(
        functools.partial(pack_body, plan, swaps_y, columns),
        [(lead, 2, span, patch), object_field.shape] + [(2, tile_rows, rim)] * swaps_y,
        [smem] + [hbm] * 2,
        [info, probe_shard, object_field],
        scratch=[dma((2 + swaps_y,))],
    )
    parts = []
    for pairs in exchanges(groups):
        block = lax.ppermute(mine, "ma", pairs)
        across = [lax.ppermute(block, "gy", p) for p in exchanges(columns)]
        parts.append([block, *across])
    (middle,) = call(
        functools.partial(widen_body, plan, swaps_y),
        [tall],
        [smem, vmem] + [vmem] * swaps_y,
        [weights_y, near_tile, *swap("gy", rims)],
    )
    probes, spectra, windows, targets, one, two = call(
        functools.partial(early_body, plan, swaps_x, groups),
        [
            (modes, 2, patch, patch),
            (units, patch, 2 * patch),
            (slots, 2, patch, patch),
            targets.shape,
            one.shape,
            two.shape,
        ],
        [smem] * 3 + [vmem] * (1 + swaps_x) + [hbm] * 4,
        [info, centres, weights_x, middle, *rows_around(middle), targets, one, two, probe_shard],
        scratch=plan.scratch(plan.narrow, False) + [dma((4,))],
        dtypes={4: jnp.bfloat16, 5: jnp.bfloat16},
    )
    packed, crossed = [], []
    for k, blocks in enumerate(parts):
        packed += call(
            join_body,
            [(columns, lead, 2, span, patch)],
            [vmem] * (columns + 1),
            [*blocks, windows if k >= UNDER else mine],
        )
        crossed += swap("gx", packed[-1:])
    probes, spectra, intensity, middle, *sends = call(
        functools.partial(start_body, plan, swaps_x, (columns, groups)),
        [probes.shape, spectra.shape, (slots, patch, patch), tall] + [fold] * swaps_x,
        [smem] * 2 + [vmem] * (6 + 2 * (groups - 1)),
        [info, centres, probes, spectra, windows, *packed, *crossed, targets, one, two],
        scratch=plan.scratch(max(plan.broad, plan.foreign), False)
        + [image_scratch, pltpu.VMEM((patch, patch), jnp.float32)],
        aliases={2: 0, 3: 1},
    )
    first_way = descent(middle, sends)
    sums, moved, change, power = call(
        functools.partial(change_body, plan, swaps_x, False),
        [(2,), (units, patch, 2 * patch), (slots, patch, patch), (slots, patch, patch)],
        [smem] * 3 + [vmem] * (5 + swaps_x),
        [info, centres, weights_x, first_way, *rows_around(first_way), spectra, probes, one, two],
        [smem] + [vmem] * 3,
        scratch=plan.scratch(plan.broad),
    )
    totals = totals_of(sums)
    spectra, first_step, middle, *sends = call(
        functools.partial(image_body, plan, swaps_x, len(totals)),
        [(units, patch, 2 * patch), (1,), tall] + [fold] * swaps_x,
        [smem] * (2 + len(totals)) + [vmem] * 9,
        [info, centres, *totals, spectra, moved, intensity, change, power, probes, targets, one, two],
        [vmem, smem] + [vmem] * (1 + swaps_x),
        scratch=plan.scratch(plan.broad) + [image_scratch],
    )
    last_way = descent(middle, sends)
    (sums,) = call(
        functools.partial(change_body, plan, swaps_x, True),
        [(2,)],
        [smem] * 3 + [vmem] * (5 + swaps_x),
        [info, centres, weights_x, last_way, *rows_around(last_way), spectra, probes, one, two],
        [smem],
        scratch=plan.scratch(plan.broad)
        + [pltpu.VMEM((slots, patch, patch), jnp.float32), pltpu.VMEM((1, 8, 128), jnp.float32)],
    )
    totals = totals_of(sums)
    (current,) = call(
        functools.partial(finish_body, plan, len(totals)),
        [(2, tile_rows, tile_cols)],
        [smem] * (len(totals) + 1) + [vmem] * 3,
        [*totals, first_step, near_tile, first_way, last_way],
        [None],
    )
    return current


def solution(mesh):
    return jax.shard_map(
        shards,
        mesh=mesh,
        in_specs=(
            P(None, "gx", "gy"),
            P("ma", None, None, None),
            P("gx", "gy", None, None, None),
            P("gx", "gy", None, None),
            P("gx", "gy"),
        ),
        out_specs=P(None, "gx", "gy"),
        check_vma=False,
    )
```
